32 devices in a mesh: groups: 2 (over x), steps: 8 (over z, y), inner: 2 (over core).
Axes of the slice: x: 2, y: 2, z: 4, core: 2. Of those that a mesh axis runs over, the one named last changes fastest.
Arguments:
- start_state: float32 [16, 32, 768], P('groups'), parts along dimension 0, may hold values from -6 to 6
- noise_draws: float32 [32, 8, 32, 768], P(('groups', 'steps', 'inner')), parts along dimension 0, may hold values from -6 to 6
- step_gaps: int32 [32], P(('groups', 'steps', 'inner')), parts along dimension 0, may hold values from 1 to 15
- window_start: int32 [2], P('groups'), parts along dimension 0, may hold values from 240 to 999
- input_weight: bfloat16 [768, 1024], replicated, may hold values from -0.21875 to 0.21875
- embed_weight: bfloat16 [256, 2048], replicated, may hold values from -0.375 to 0.375
- first_weight: bfloat16 [1024, 1024], replicated, may hold values from -0.1875 to 0.1875
- second_weight: bfloat16 [1024, 1024], replicated, may hold values from -0.1875 to 0.1875
- output_weight: bfloat16 [1024, 768], replicated, may hold values from -0.1875 to 0.1875
Outputs:
- trajectory: float32 [32, 8, 32, 768], P(('groups', 'steps', 'inner')), parts along dimension 0
The draws below stay inside these ranges and needn't reach their ends.
There are 2 independent parts, one for each index of `groups`. The reference program is written for one: setup_inputs(seed, part) draws one part's arguments, and reference() takes and returns one part's arrays. A program takes and returns all parts, laid end to end along the dimension named above; an argument that names none is the same for every part. Nothing has to cross between parts.
All inputs are finite; a program needn't handle non-finite values.
Results may differ from the reference program's by a relative error of at most 0.00035.
Values sent between devices are 32-bit elements; how exact they have to be, the bound alone decides.
A program may use at most 64 MiB of HBM per device.

```python
import math
import jax
import jax.numpy as jnp
from jax import lax

BATCH = 8
PATCHES = 32
FEATURES = 768
CHANNELS = 1024
FREQS = 128
GROUPS = 32
ITERS = 2
GAP_MAX = 15
TRAIN_STEPS = 1000
WINDOW = 16


def place_ends(array, rng, low, high):
    place = [jax.random.randint(jax.random.fold_in(rng, axis), (), 0, length) for axis, length in enumerate(array.shape)]
    main_axis = array.shape.index(max(array.shape))
    neighbour = place[:main_axis] + [(place[main_axis] + 1) % array.shape[main_axis]] + place[main_axis + 1:]
    return array.at[tuple(place)].set(low).at[tuple(neighbour)].set(high)


def shard_levels(stream_key, dims, split, least, largest):
    def one(position, shards_of):
        heights = jax.random.uniform(jax.random.fold_in(jax.random.fold_in(stream_key, 6), position), (shards_of,), jnp.float32, least / len(split), largest / len(split))
        return jnp.repeat(jnp.exp(heights), dims[position] // shards_of).reshape((-1,) + (1,) * (len(dims) - position - 1))

    level = one(*split[0])
    for cut in split[1:]:
        level = level * one(*cut)
    return level


def scatter_about(own_key, shape, deviation, bound, cuts=(), held_as=jnp.bfloat16):
    drawn = deviation * jax.random.normal(own_key, shape, jnp.float32)
    if cuts:
        drawn = drawn * shard_levels(own_key, shape, cuts, -0.22, 0.18)
    return jnp.clip(drawn, -bound, bound).astype(held_as)


def setup_inputs(seed: int = 0, part: int = 0) -> dict:
    key_list = jax.random.split(jax.random.key(seed), 10)
    part_keys = jax.random.split(jax.random.fold_in(key_list[9], part), 10)
    start_state = scatter_about(part_keys[0], (BATCH, PATCHES, FEATURES), 1.0, 6.0, (), jnp.float32)
    noise_draws = scatter_about(part_keys[1], (WINDOW, BATCH, PATCHES, FEATURES), 1.0, 6.0, ((0, 16),), jnp.float32)
    step_gaps = place_ends(jax.random.randint(part_keys[2], (WINDOW,), 1, GAP_MAX + 1), jax.random.fold_in(part_keys[2], 1), 1, GAP_MAX).astype(jnp.int32)
    window_start = jax.random.randint(part_keys[3], (1,), WINDOW * GAP_MAX, TRAIN_STEPS).astype(jnp.int32)
    input_weight = scatter_about(key_list[4], (FEATURES, CHANNELS), FEATURES ** -0.5, 0.21875)
    embed_weight = scatter_about(key_list[5], (2 * FREQS, 2 * CHANNELS), (2 * FREQS) ** -0.5, 0.375)
    first_weight = scatter_about(key_list[6], (CHANNELS, CHANNELS), CHANNELS ** -0.5, 0.1875)
    second_weight = scatter_about(key_list[7], (CHANNELS, CHANNELS), CHANNELS ** -0.5, 0.1875)
    output_weight = scatter_about(key_list[8], (CHANNELS, FEATURES), CHANNELS ** -0.5, 0.1875)
    return dict(start_state=start_state, noise_draws=noise_draws, step_gaps=step_gaps, window_start=window_start, input_weight=input_weight, embed_weight=embed_weight, first_weight=first_weight, second_weight=second_weight, output_weight=output_weight)


def noise_table():
    levels = jnp.arange(TRAIN_STEPS, dtype=jnp.float32)
    beta_values = 0.0001 + (0.02 - 0.0001) * levels / (TRAIN_STEPS - 1)
    return jnp.exp(jnp.cumsum(jnp.log1p(-beta_values)))

def lookup(table, noise_level):
    places = jnp.arange(TRAIN_STEPS, dtype=jnp.int32)
    return jnp.sum(jnp.where(places == noise_level, table, jnp.zeros_like(table)))

def group_norm(hidden, batch_count):
    total_rows, channel_count = hidden.shape
    shaped = hidden.reshape(batch_count, total_rows // batch_count, channel_count)

    def group_mean(values):
        per_channel = lax.optimization_barrier(jnp.mean(values, axis=1)).reshape(batch_count, GROUPS, channel_count // GROUPS)
        per_group = lax.optimization_barrier(jnp.mean(per_channel, axis=2, keepdims=True))
        return jnp.broadcast_to(per_group, per_channel.shape).reshape(batch_count, 1, channel_count)
    center = group_mean(shaped)
    offset = shaped - center
    spread = group_mean(offset * offset)
    return (offset * lax.rsqrt(spread + 1e-05)).reshape(total_rows, channel_count)

def predict_noise(state, noise_level, input_weight, embed_weight, first_weight, second_weight, output_weight):
    batch_count, patch_count, feature_count = state.shape
    channel_count = input_weight.shape[1]
    flat_state = state.reshape(batch_count * patch_count, feature_count).astype(jnp.bfloat16)
    entry_hidden = jnp.dot(flat_state, input_weight, preferred_element_type=jnp.float32)
    half_count = embed_weight.shape[0] // 2
    frequency = jnp.exp(-math.log(10000.0) * jnp.arange(half_count, dtype=jnp.float32) / half_count)
    angles = noise_level.astype(jnp.float32) * frequency
    features = jnp.concatenate([jnp.cos(angles), jnp.sin(angles)])[None, :].astype(jnp.bfloat16)
    modulation = jnp.dot(features, embed_weight, preferred_element_type=jnp.float32)
    scale_part = modulation[:, :channel_count]
    shift_part = modulation[:, channel_count:]
    act_one = jax.nn.silu(group_norm(entry_hidden, batch_count) * (1.0 + scale_part) + shift_part).astype(jnp.bfloat16)
    middle = jnp.dot(act_one, first_weight, preferred_element_type=jnp.float32)
    act_two = jax.nn.silu(group_norm(middle, batch_count)).astype(jnp.bfloat16)
    block_out = entry_hidden + jnp.dot(act_two, second_weight, preferred_element_type=jnp.float32)
    act_three = jax.nn.silu(group_norm(block_out, batch_count)).astype(jnp.bfloat16)
    predicted = jnp.dot(act_three, output_weight, preferred_element_type=jnp.float32)
    return predicted.reshape(state.shape)

def drift_of(state, noise_draw, level_now, level_next, table, input_weight, embed_weight, first_weight, second_weight, output_weight):
    predicted = predict_noise(state, level_now, input_weight, embed_weight, first_weight, second_weight, output_weight)
    bar_now = lookup(table, level_now)
    bar_next = lookup(table, level_next)
    clean_guess = jnp.clip((state - jnp.sqrt(1.0 - bar_now) * predicted) / jnp.sqrt(bar_now), -1.0, 1.0)
    implied = (state - jnp.sqrt(bar_now) * clean_guess) / jnp.sqrt(1.0 - bar_now)
    sigma_value = jnp.sqrt((1.0 - bar_next) / (1.0 - bar_now) * (1.0 - bar_now / bar_next))
    noise_coef = (1.0 - bar_next) * jnp.sqrt(bar_now / (bar_next * (1.0 - bar_now)))
    return jnp.sqrt(bar_next) * clean_guess + noise_coef * implied + sigma_value * noise_draw - state

def reference(start_state, noise_draws, step_gaps, window_start, input_weight, embed_weight, first_weight, second_weight, output_weight):
    table = noise_table()
    before = jnp.cumsum(step_gaps) - step_gaps
    level_now = (window_start[0] - before).astype(jnp.int32)
    level_next = (level_now - step_gaps).astype(jnp.int32)
    states = jnp.broadcast_to(start_state[None], noise_draws.shape)

    def one_step(item):
        return drift_of(item[0], item[1], item[2], item[3], table, input_weight, embed_weight, first_weight, second_weight, output_weight)
    totals = states
    for iteration in range(ITERS):
        drifts = lax.map(one_step, (states, noise_draws, level_now, level_next))
        totals = jnp.cumsum(drifts, axis=0)
        states = start_state[None] + (totals - drifts)
    return start_state[None] + totals
```

```python
import functools
import math

import jax
import jax.numpy as jnp
import numpy as np
from jax import lax
from jax.experimental import pallas as pl
from jax.experimental.pallas import tpu as pltpu
from jax.sharding import PartitionSpec as P

GROUPS = 32
PIECES = 2
FIRST = ((0, 1),)
SECOND = ((0,), (1,))
ITERS = 2
TRAIN_STEPS = 1000
LANES = 128
BLOCK = 256
MESH = pl.DeviceIdType.MESH
F32 = jnp.float32
BF16 = jnp.bfloat16


def noise_table():
    levels = np.arange(TRAIN_STEPS, dtype=np.float32)
    beta = (0.0001 + (0.02 - 0.0001) * levels / (TRAIN_STEPS - 1)).astype(np.float32)
    bars = np.exp(np.cumsum(np.log1p(-beta.astype(np.float64)))).astype(np.float32)
    padded = np.zeros((-(-TRAIN_STEPS // (8 * LANES)) * 8 * LANES,), np.float32)
    padded[:TRAIN_STEPS] = bars
    return padded.reshape(-1, LANES)


def frequencies(count):
    powers = -math.log(10000.0) * np.arange(count, dtype=np.float32) / count
    return np.exp(powers.astype(np.float32)).astype(np.float32)[None, :]


def group_matrix(channels, rows):
    width = channels // GROUPS
    place = np.arange(BLOCK) // width
    same = (place[:, None] == place[None, :]).astype(np.float32)
    return same / (width * rows)


def silu(value):
    half = 0.5 * value
    return half + half * jnp.tanh(half)


def kernel(
    cfg,
    gap_ref,
    start_level_ref,
    table_ref,
    freq_ref,
    group_ref,
    start_hbm,
    noise_hbm,
    win_hbm,
    wemb_hbm,
    w1_hbm,
    w2_hbm,
    wout_hbm,
    out_v,
    start_v,
    noise_v,
    noise_all,
    win,
    wemb,
    w1,
    w2,
    wout,
    gap_send,
    gap_all,
    base_rx,
    base_tx,
    modulation_v,
    coef_v,
    part_v,
    state_v,
    chain_rx,
    chain_tx,
    out_tx,
    load_sem,
    gap_send_sem,
    gap_recv_sem,
    base_sem,
    noise_send,
    noise_recv,
    chain_send,
    chain_recv,
    out_send,
    out_recv,
):
    steps, inner, columns, own, patches, features, channels = cfg
    rows = steps // columns
    plane = columns * inner
    s = lax.axis_index("steps")
    h = lax.axis_index("inner")
    z = s // columns
    p = lax.rem(s, columns) * inner + h
    first = p * own

    def load(i, src, dst):
        return pltpu.make_async_copy(src, dst, load_sem.at[i])

    loads = [
        load(0, noise_hbm, noise_v),
        load(1, start_hbm.at[pl.ds(first, own)], start_v),
        load(2, win_hbm, win),
        load(3, noise_hbm.at[pl.ds(first, own)], noise_all.at[p]),
        load(4, wemb_hbm, wemb),
        load(5, w1_hbm, w1),
        load(6, w2_hbm, w2),
        load(7, wout_hbm, wout),
    ]
    for copy in loads:
        copy.start()

    def mate(r):
        q = lax.rem(p + r, plane)
        return q, {"steps": z * columns + q // inner, "inner": lax.rem(q, inner)}

    below, above = {"steps": s - columns}, {"steps": s + columns}

    barrier = pltpu.get_barrier_semaphore()
    for r in range(1, plane):
        pl.semaphore_signal(barrier, inc=1, device_id=mate(r)[1], device_id_type=MESH)

    @pl.when(z > 0)
    def _():
        pl.semaphore_signal(barrier, inc=1, device_id=below, device_id_type=MESH)

    @pl.when(z < rows - 1)
    def _():
        pl.semaphore_signal(barrier, inc=1, device_id=above, device_id_type=MESH)

    gap_send[...] = jnp.zeros_like(gap_send) + gap_ref[0]
    gap_all[p] = jnp.zeros_like(gap_send) + gap_ref[0]

    @pl.when(z == 0)
    def _():
        base_rx[...] = jnp.zeros_like(base_rx)
        chain_rx[...] = jnp.zeros_like(chain_rx)

    neighbours = (z + rows - 1) // rows + (2 * rows - 2 - z) // rows
    pl.semaphore_wait(barrier, plane - 1 + neighbours)

    def gap_copy(r, slot):
        return pltpu.make_async_remote_copy(
            src_ref=gap_send,
            dst_ref=gap_all.at[slot],
            send_sem=gap_send_sem.at[r],
            recv_sem=gap_recv_sem.at[slot],
            device_id=mate(r)[1],
            device_id_type=MESH,
        )

    def base_copy():
        return pltpu.make_async_remote_copy(
            src_ref=base_tx,
            dst_ref=base_rx,
            send_sem=base_sem.at[0],
            recv_sem=base_sem.at[1],
            device_id=above,
            device_id_type=MESH,
        )

    def noise_copy(j, r, slot):
        q, device = mate(r)
        return pltpu.make_async_remote_copy(
            src_ref=noise_v.at[q * own + j],
            dst_ref=noise_all.at[slot, j],
            send_sem=noise_send.at[j, r],
            recv_sem=noise_recv.at[slot, j],
            device_id=device,
            device_id_type=MESH,
        )

    def out_copy(j, r, slot):
        q, device = mate(r)
        return pltpu.make_async_remote_copy(
            src_ref=out_tx.at[j, q],
            dst_ref=out_v.at[slot * own + j],
            send_sem=out_send.at[j, r],
            recv_sem=out_recv.at[slot, j],
            device_id=device,
            device_id_type=MESH,
        )

    depth = patches // PIECES

    def chain_copy(n, j, q):
        cut = pl.ds(q * depth, depth)
        return pltpu.make_async_remote_copy(
            src_ref=chain_tx.at[n, j, cut],
            dst_ref=chain_rx.at[n, j, cut],
            send_sem=chain_send.at[n, j, q],
            recv_sem=chain_recv.at[n, j, q],
            device_id=above,
            device_id_type=MESH,
        )

    for r in range(1, plane):
        gap_copy(r, p).start()
    loads[0].wait()
    for j in range(own):
        for r in range(1, plane):
            noise_copy(j, r, p).start()

    def group_average(partial, size):
        blocks = channels // BLOCK
        stacked = jnp.concatenate(
            [partial[:, i * BLOCK : (i + 1) * BLOCK] for i in range(blocks)], axis=0
        )
        matrix = group_ref[...]
        high = stacked.astype(BF16)
        rest = stacked - high.astype(F32)
        middle = rest.astype(BF16)
        low = (rest - middle.astype(F32)).astype(BF16)
        parts = jnp.concatenate([low, middle, high], axis=0)
        summed = jnp.dot(parts, matrix, preferred_element_type=F32)
        summed = jnp.sum(summed.reshape(3, -1, BLOCK), axis=0)
        summed = jnp.sum(summed.reshape(blocks, size, 8, BLOCK), axis=2, keepdims=True)
        return jnp.concatenate([summed[i] for i in range(blocks)], axis=-1)

    def row_sums(value, size):
        return jnp.sum(value.reshape(size, patches // 8, 8, channels), axis=1).reshape(
            size * 8, channels
        )

    def centered(hidden, size):
        shaped = hidden.reshape(size, patches, channels)
        offset = shaped - group_average(row_sums(shaped, size), size)
        return offset, lax.rsqrt(group_average(row_sums(offset * offset, size), size) + 1e-05)

    def project(value, weight):
        return jnp.dot(value, weight[...], preferred_element_type=F32)

    def set_levels():
        for r in range(1, plane):
            slot = mate(r)[0]
            gap_copy(r, slot).wait_recv()

        @pl.when(z > 0)
        def _():
            base_copy().wait_recv()

        gaps = [gap_all[t] for t in range(plane)]
        base = base_rx[...]
        total = base
        for gap in gaps:
            total = total + gap
        base_tx[...] = total

        @pl.when(z < rows - 1)
        def _():
            base_copy().start()

        table = table_ref[...]
        tall = lax.broadcasted_iota(jnp.int32, table.shape, 0)
        places = tall * LANES + lax.broadcasted_iota(jnp.int32, table.shape, 1)
        level = start_level_ref[0] - base
        levels = [level]
        for gap in gaps:
            level = level - gap
            levels.append(level)

        def lookup(level):
            found = jnp.where(places == level[:1, :1], table, 0.0)
            return jnp.sum(jnp.sum(found, axis=0, keepdims=True), axis=1, keepdims=True)

        bars = [lookup(level) for level in levels]
        bar_now, bar_next = jnp.ones(table.shape, F32), jnp.ones(table.shape, F32)
        level_now = levels[0]
        for t in range(plane):
            bar_now = jnp.where(tall == t, bars[t], bar_now)
            bar_next = jnp.where(tall == t, bars[t + 1], bar_next)
            level_now = jnp.where(tall == t, levels[t], level_now)
        coefs = [
            jnp.sqrt(1.0 - bar_now),
            1.0 / jnp.sqrt(bar_now),
            jnp.sqrt(bar_now),
            1.0 / jnp.sqrt(1.0 - bar_now),
            jnp.sqrt(bar_next),
            (1.0 - bar_next) * jnp.sqrt(bar_now / (bar_next * (1.0 - bar_now))),
            jnp.sqrt((1.0 - bar_next) / (1.0 - bar_now) * (1.0 - bar_now / bar_next)),
        ]
        for i, coef in enumerate(coefs):
            coef_v[i] = coef
        angles = level_now.astype(F32) * freq_ref[...]
        around = jnp.concatenate([jnp.cos(angles), jnp.sin(angles)], axis=1).astype(BF16)
        loads[4].wait()
        modulation_v[...] = project(around, wemb)

    def modulations(low):
        return jnp.concatenate(
            [modulation_v[t : t + 1, low : low + channels] for t in range(plane)], axis=0
        ).reshape(plane, 1, channels)

    def drifts(n, j, eps):
        result = []
        for t in range(plane):
            state = start_v[j] if n == 0 else state_v[j, t]
            coef = [coef_v[i][t : t + 1, :1] for i in range(7)]
            clean = jnp.clip((state - coef[0] * eps[t]) * coef[1], -1.0, 1.0)
            implied = (state - coef[2] * clean) * coef[3]
            result.append(coef[4] * clean + coef[5] * implied + coef[6] * noise_all[t, j] - state)
        return result

    def forward(n, j):
        for q in range(PIECES):
            cut = pl.ds(q * depth, depth)
            chain_copy(n, j, q).wait_recv()
            chain_tx[n, j, cut] = chain_tx[n, j, cut] + chain_rx[n, j, cut]

            @pl.when(z < rows - 1)
            def _():
                chain_copy(n, j, q).start()

    def launch(n, j):
        for q in range(PIECES):
            chain_copy(n, j, q).start()

    def denoise(n, group, entries, entry_norms, between):
        scale, shift = 1.0 + modulations(0), modulations(channels)
        ones = []
        for offset, spread in entry_norms:
            ones.append(silu(offset * (spread * scale) + shift).astype(BF16))
        if n == 0:
            loads[5].wait()
        middles = [project(one.reshape(-1, channels), w1) for one in ones]
        twos = []
        for middle in middles:
            offset, spread = centered(middle, plane)
            twos.append(silu(offset * spread).astype(BF16))
        if n == 0:
            loads[6].wait()
        blocks = []
        for entry, two in zip(entries, twos):
            added = project(two.reshape(-1, channels), w2).reshape(plane, patches, channels)
            blocks.append(entry + added)
        threes = []
        for block in blocks:
            offset, spread = centered(block, plane)
            threes.append(silu(offset * spread).astype(BF16))
        if n == 0:
            loads[7].wait()
        for j, three in zip(group, threes):
            eps = project(three.reshape(-1, channels), wout).reshape(plane, patches, features)
            between(j)
            finish(n, j, eps)

    def finish(n, j, eps):
        steps_of = drifts(n, j, eps)
        running = steps_of[0]
        if n == 0:
            for t in range(1, plane):
                part_v[j, t] = running
                running = running + steps_of[t]
            chain_tx[n, j] = running

            @pl.when(z == 0)
            def _():
                launch(n, j)
        else:
            origin = start_v[j]
            out_tx[j, 0] = origin + running
            for t in range(1, plane):
                running = running + steps_of[t]
                out_tx[j, t] = origin + running
            chain_tx[n, j] = running

            @pl.when(z == 0)
            def _():
                launch(n, j)

            @pl.when(z > 0)
            def _():
                forward(n, j)
                earlier = chain_rx[n, j]
                for t in range(plane):
                    out_tx[j, t] = out_tx[j, t] + earlier

            for r in range(1, plane):
                out_copy(j, r, p).start()
            out_v[first + j] = out_tx[j, p]

    loads[1].wait()
    loads[2].wait()
    flat = start_v[...].reshape(own * patches, features).astype(BF16)
    entry = project(flat, win)
    offset, spread = centered(entry, own)
    shaped = entry.reshape(own, patches, channels)
    set_levels()

    def noise_arrives(j):
        if j == 0:
            loads[3].wait()
        for r in range(1, plane):
            slot = mate(r)[0]
            noise_copy(j, r, slot).wait_recv()

    for group in FIRST:
        denoise(
            0,
            group,
            [shaped[j : j + 1] for j in group],
            [(offset[j : j + 1], spread[j : j + 1]) for j in group],
            noise_arrives,
        )

    @pl.when(z > 0)
    def _():
        for j in range(own):
            forward(0, j)

    for group in SECOND:
        entries, norms = [], []
        for j in group:
            state_v[j, 0] = start_v[j] + chain_rx[0, j]
            for t in range(1, plane):
                state_v[j, t] = start_v[j] + (chain_rx[0, j] + part_v[j, t])
            flat = state_v[j].reshape(plane * patches, features).astype(BF16)
            entry = project(flat, win)
            entries.append(entry.reshape(plane, patches, channels))
            norms.append(centered(entry, plane))
        denoise(1, group, entries, norms, lambda j: None)

    for r in range(1, plane):
        slot = mate(r)[0]
        for j in range(own):
            out_copy(j, r, slot).wait_recv()

    for r in range(1, plane):
        gap_copy(r, p).wait_send()
        for j in range(own):
            noise_copy(j, r, p).wait_send()
            out_copy(j, r, p).wait_send()

    @pl.when(z < rows - 1)
    def _():
        base_copy().wait_send()
        for n in range(ITERS):
            for j in range(own):
                for q in range(PIECES):
                    chain_copy(n, j, q).wait_send()


def shards(
    steps,
    inner,
    start_state,
    noise_draws,
    step_gaps,
    window_start,
    input_weight,
    embed_weight,
    first_weight,
    second_weight,
    output_weight,
):
    batch, patches, features = start_state.shape
    channels = input_weight.shape[1]
    columns = 2 if steps % 2 == 0 else 1
    plane = columns * inner
    own = batch // plane
    cfg = (steps, inner, columns, own, patches, features, channels)
    image = (patches, features)
    table = jnp.asarray(noise_table())
    freq = jnp.asarray(frequencies(embed_weight.shape[0] // 2))
    matrix = jnp.asarray(group_matrix(channels, patches)).astype(BF16)
    smem = pl.BlockSpec(memory_space=pltpu.SMEM)
    vmem = pl.BlockSpec(memory_space=pltpu.VMEM)
    anywhere = pl.BlockSpec(memory_space=pltpu.HBM)
    dma = pltpu.SemaphoreType.DMA
    out = pl.pallas_call(
        functools.partial(kernel, cfg),
        out_shape=pltpu.VMEM((batch,) + image, F32),
        in_specs=[smem, smem, vmem, vmem, vmem] + [anywhere] * 7,
        out_specs=vmem,
        scratch_shapes=[
            pltpu.VMEM((own,) + image, F32),
            pltpu.VMEM((batch,) + image, F32),
            pltpu.VMEM((plane, own) + image, F32),
            pltpu.VMEM(input_weight.shape, BF16),
            pltpu.VMEM(embed_weight.shape, BF16),
            pltpu.VMEM(first_weight.shape, BF16),
            pltpu.VMEM(second_weight.shape, BF16),
            pltpu.VMEM(output_weight.shape, BF16),
            pltpu.VMEM((8, LANES), jnp.int32),
            pltpu.VMEM((plane, 8, LANES), jnp.int32),
            pltpu.VMEM((8, LANES), jnp.int32),
            pltpu.VMEM((8, LANES), jnp.int32),
            pltpu.VMEM((8, 2 * channels), F32),
            pltpu.VMEM((7, 8, LANES), F32),
            pltpu.VMEM((own, plane) + image, F32),
            pltpu.VMEM((own, plane) + image, F32),
            pltpu.VMEM((ITERS, own) + image, F32),
            pltpu.VMEM((ITERS, own) + image, F32),
            pltpu.VMEM((own, plane) + image, F32),
            dma((8,)),
            dma((plane,)),
            dma((plane,)),
            dma((2,)),
            dma((own, plane)),
            dma((plane, own)),
            dma((ITERS, own, PIECES)),
            dma((ITERS, own, PIECES)),
            dma((own, plane)),
            dma((plane, own)),
        ],
        compiler_params=pltpu.CompilerParams(
            collective_id=0, has_side_effects=True, vmem_limit_bytes=56 * 1024 * 1024
        ),
    )(
        step_gaps,
        window_start,
        table,
        freq,
        matrix,
        start_state,
        noise_draws.reshape((batch,) + image),
        input_weight,
        embed_weight,
        first_weight,
        second_weight,
        output_weight,
    )
    return out.reshape((1,) + start_state.shape)


def solution(mesh):
    steps, inner = mesh.shape["steps"], mesh.shape["inner"]
    return jax.shard_map(
        functools.partial(shards, steps, inner),
        mesh=mesh,
        in_specs=(
            P("groups", None, None),
            P(("groups", "steps", "inner"), None, None, None),
            P(("groups", "steps", "inner")),
            P("groups"),
            P(),
            P(),
            P(),
            P(),
            P(),
        ),
        out_specs=P(("groups", "steps", "inner"), None, None, None),
        check_vma=False,
    )
```

```python
import functools
import math

import jax
import jax.numpy as jnp
import numpy as np
from jax import lax
from jax.experimental import pallas as pl
from jax.experimental.pallas import tpu as pltpu
from jax.sharding import PartitionSpec as P

GROUPS = 32
PIECES = 4
OUTER_ONE = False
OUTER_TWO = False
ITERS = 2
TRAIN_STEPS = 1000
LANES = 128
BLOCK = 256
MESH = pl.DeviceIdType.MESH
F32 = jnp.float32
BF16 = jnp.bfloat16


def noise_table():
    levels = np.arange(TRAIN_STEPS, dtype=np.float32)
    beta = (0.0001 + (0.02 - 0.0001) * levels / (TRAIN_STEPS - 1)).astype(np.float32)
    bars = np.exp(np.cumsum(np.log1p(-beta.astype(np.float64)))).astype(np.float32)
    padded = np.zeros((-(-TRAIN_STEPS // (8 * LANES)) * 8 * LANES,), np.float32)
    padded[:TRAIN_STEPS] = bars
    return padded.reshape(-1, LANES)


def frequencies(count):
    powers = -math.log(10000.0) * np.arange(count, dtype=np.float32) / count
    return np.exp(powers.astype(np.float32)).astype(np.float32)[None, :]


def group_matrix(channels, rows):
    width = channels // GROUPS
    place = np.arange(BLOCK) // width
    same = (place[:, None] == place[None, :]).astype(np.float32)
    return same / (width * rows)


def silu_of_half(half):
    return half + half * jnp.tanh(half)


def kernel(
    cfg,
    gap_hbm,
    start_level_hbm,
    table_hbm,
    freq_hbm,
    group_hbm,
    start_hbm,
    noise_hbm,
    win_hbm,
    wemb_hbm,
    w1_hbm,
    w2_hbm,
    wout_hbm,
    out_v,
    gap_ref,
    start_level_ref,
    table_ref,
    freq_ref,
    group_ref,
    start_v,
    noise_v,
    noise_all,
    win,
    wemb,
    w1,
    w2,
    wout,
    gap_send,
    gap_all,
    base_rx,
    base_tx,
    modulation_v,
    coef_v,
    part_v,
    state_v,
    chain_rx,
    chain_tx,
    out_tx,
    eps_v,
    load_sem,
    gap_send_sem,
    gap_recv_sem,
    base_sem,
    noise_send,
    noise_recv,
    chain_send,
    chain_recv,
    out_send,
    out_recv,
):
    steps, inner, columns, own, patches, features, channels = cfg
    rows = steps // columns
    plane = columns * inner
    s = lax.axis_index("steps")
    h = lax.axis_index("inner")
    z = s // columns
    p = lax.rem(s, columns) * inner + h
    first = p * own

    def load(i, src, dst):
        return pltpu.make_async_copy(src, dst, load_sem.at[i])

    loads = [
        load(0, noise_hbm, noise_v),
        load(1, start_hbm.at[pl.ds(first, own)], start_v),
        load(2, win_hbm, win),
        load(3, noise_hbm.at[pl.ds(first, own)], noise_all.at[p]),
        load(4, wemb_hbm, wemb),
        load(5, w1_hbm, w1),
        load(6, w2_hbm, w2),
        load(7, wout_hbm, wout),
        load(8, gap_hbm, gap_ref),
        load(9, start_level_hbm, start_level_ref),
        load(10, table_hbm, table_ref),
        load(11, freq_hbm, freq_ref),
        load(12, group_hbm, group_ref),
    ]
    def mate(r):
        q = lax.rem(p + r, plane)
        return q, {"steps": z * columns + q // inner, "inner": lax.rem(q, inner)}

    below, above = {"steps": s - columns}, {"steps": s + columns}

    barrier = pltpu.get_barrier_semaphore()
    for r in range(1, plane):
        pl.semaphore_signal(barrier, inc=1, device_id=mate(r)[1], device_id_type=MESH)

    @pl.when(z > 0)
    def _():
        pl.semaphore_signal(barrier, inc=1, device_id=below, device_id_type=MESH)

    @pl.when(z < rows - 1)
    def _():
        pl.semaphore_signal(barrier, inc=1, device_id=above, device_id_type=MESH)

    for i in (8, 0, 9, 10, 11, 1, 2, 12, 3, 4, 5, 6, 7):
        loads[i].start()

    loads[8].wait()
    gap_send[...] = jnp.zeros_like(gap_send) + gap_ref[0]
    gap_all[p] = jnp.zeros_like(gap_send) + gap_ref[0]

    @pl.when(z == 0)
    def _():
        base_rx[...] = jnp.zeros_like(base_rx)
        chain_rx[...] = jnp.zeros_like(chain_rx)

    neighbours = (z + rows - 1) // rows + (2 * rows - 2 - z) // rows
    pl.semaphore_wait(barrier, plane - 1 + neighbours)

    def gap_copy(r, slot):
        return pltpu.make_async_remote_copy(
            src_ref=gap_send,
            dst_ref=gap_all.at[slot],
            send_sem=gap_send_sem.at[r],
            recv_sem=gap_recv_sem.at[slot],
            device_id=mate(r)[1],
            device_id_type=MESH,
        )

    def base_copy():
        return pltpu.make_async_remote_copy(
            src_ref=base_tx,
            dst_ref=base_rx,
            send_sem=base_sem.at[0],
            recv_sem=base_sem.at[1],
            device_id=above,
            device_id_type=MESH,
        )

    def noise_copy(j, r, slot):
        q, device = mate(r)
        return pltpu.make_async_remote_copy(
            src_ref=noise_v.at[q * own + j],
            dst_ref=noise_all.at[slot, j],
            send_sem=noise_send.at[j, r],
            recv_sem=noise_recv.at[slot, j],
            device_id=device,
            device_id_type=MESH,
        )

    depth = patches // PIECES

    def out_copy(j, r, slot, piece):
        q, device = mate(r)
        cut = pl.ds(piece * depth, depth)
        return pltpu.make_async_remote_copy(
            src_ref=out_tx.at[j, q, cut],
            dst_ref=out_v.at[slot * own + j, cut],
            send_sem=out_send.at[j, r, piece],
            recv_sem=out_recv.at[slot, j, piece],
            device_id=device,
            device_id_type=MESH,
        )

    def chain_copy(n, j, q):
        cut = pl.ds(q * depth, depth)
        return pltpu.make_async_remote_copy(
            src_ref=chain_tx.at[n, j, cut],
            dst_ref=chain_rx.at[n, j, cut],
            send_sem=chain_send.at[n, j, q],
            recv_sem=chain_recv.at[n, j, q],
            device_id=above,
            device_id_type=MESH,
        )

    for r in range(1, plane):
        gap_copy(r, p).start()
    loads[0].wait()
    for j in range(own):
        for r in range(1, plane):
            noise_copy(j, r, p).start()

    def cut_columns(value):
        return [value[..., i : i + BLOCK] for i in range(0, value.shape[-1], BLOCK)]

    def pack(partial):
        row = lax.broadcasted_iota(jnp.int32, (8, BLOCK), 0)
        top, late = row < 4, lax.rem(row, 4) >= 2
        packed = []
        for i in range(0, partial.shape[0], 4):
            a, b, c, d = (partial[i + k] for k in range(4))
            ab = jnp.where(top, a, b) + pltpu.roll(jnp.where(top, b, a), 4, 0)
            cd = jnp.where(top, c, d) + pltpu.roll(jnp.where(top, d, c), 4, 0)
            four = jnp.where(late, ab + pltpu.roll(ab, 2, 0), cd + pltpu.roll(cd, 6, 0))
            packed.append(four + pltpu.roll(four, 1, 0))
        return packed

    def group_averages(partials):
        size = partials[0].shape[0]
        whole = size % 4 == 0
        rows = []
        for partial in partials:
            rows.extend(pack(partial) if whole else [partial.reshape(size * 8, BLOCK)])
        rows = jnp.concatenate(rows, axis=0)
        high = rows.astype(BF16).astype(F32)
        rest = rows - high
        middle = rest.astype(BF16).astype(F32)
        parts = jnp.concatenate([rest - middle, middle, high], axis=0).astype(BF16)
        summed = jnp.dot(parts, group_ref[...], preferred_element_type=F32)
        summed = jnp.sum(summed.reshape(3, len(partials), -1, BLOCK), axis=0)
        if not whole:
            summed = summed.reshape(len(partials), size, 8, BLOCK)
            return list(jnp.sum(summed, axis=2, keepdims=True))
        places = [i // 4 * 8 + (3, 7, 1, 5)[i % 4] for i in range(size)]
        return [jnp.stack([block[r : r + 1] for r in places], axis=0) for block in summed]

    def row_sums(value):
        size = value.shape[0]
        return jnp.sum(value.reshape(size, patches // 8, 8, BLOCK), axis=1)

    def pivots(block):
        rows = block[:, 0, :]
        lane = lax.broadcasted_iota(jnp.int32, (rows.shape[0], LANES), 1)
        lead = lane - lax.rem(lane, channels // GROUPS)
        halves = [
            jnp.take_along_axis(rows[:, i : i + LANES], lead, axis=1)
            for i in range(0, BLOCK, LANES)
        ]
        return jnp.concatenate(halves, axis=1)[:, None, :]

    def centered(block):
        shifted = block - pivots(block)
        mean, square = group_averages([row_sums(shifted), row_sums(shifted * shifted)])
        return shifted, mean, lax.rsqrt(jnp.maximum(square - mean * mean, 0.0) + 1e-05)

    def project(acts, weight, outer=True):
        sums = [None] * (weight.shape[1] // BLOCK)
        pairs = [(k, n) for k in range(len(acts)) for n in range(len(sums))]
        if not outer:
            pairs = [(k, n) for n in range(len(sums)) for k in range(len(acts))]
        for k, n in pairs:
            tile = weight[pl.ds(k * BLOCK, BLOCK), pl.ds(n * BLOCK, BLOCK)]
            part = jnp.dot(acts[k], tile, preferred_element_type=F32)
            sums[n] = part if sums[n] is None else sums[n] + part
        return sums

    def shape_images(blocks, size):
        return [block.reshape(size, patches, BLOCK) for block in blocks]

    def flatten(value):
        return value.reshape(-1, BLOCK).astype(BF16)

    def activate(blocks):
        result = []
        for block in blocks:
            shifted, mean, spread = centered(block)
            gain = 0.5 * spread
            result.append(flatten(silu_of_half(shifted * gain - mean * gain)))
        return result

    def set_levels():
        for r in range(1, plane):
            slot = mate(r)[0]
            gap_copy(r, slot).wait_recv()

        @pl.when(z > 0)
        def _():
            base_copy().wait_recv()

        gaps = [gap_all[t] for t in range(plane)]
        base = base_rx[...]
        total = base
        for gap in gaps:
            total = total + gap
        base_tx[...] = total

        @pl.when(z < rows - 1)
        def _():
            base_copy().start()

        for i in (9, 10, 11):
            loads[i].wait()
        table = table_ref[...]
        tall = lax.broadcasted_iota(jnp.int32, table.shape, 0)
        places = tall * LANES + lax.broadcasted_iota(jnp.int32, table.shape, 1)
        level = start_level_ref[0] - base
        levels = [level]
        for gap in gaps:
            level = level - gap
            levels.append(level)

        def lookup(level):
            found = jnp.where(places == level[:1, :1], table, 0.0)
            return jnp.sum(jnp.sum(found, axis=0, keepdims=True), axis=1, keepdims=True)

        bars = [lookup(level) for level in levels]
        bar_now, bar_next = jnp.ones(table.shape, F32), jnp.ones(table.shape, F32)
        level_now = levels[0]
        for t in range(plane):
            bar_now = jnp.where(tall == t, bars[t], bar_now)
            bar_next = jnp.where(tall == t, bars[t + 1], bar_next)
            level_now = jnp.where(tall == t, levels[t], level_now)
        rest = 1.0 - bar_now
        lift = (1.0 - bar_next) * jnp.sqrt(bar_now / (bar_next * rest)) / jnp.sqrt(rest)
        coefs = [
            1.0 / jnp.sqrt(bar_now),
            jnp.sqrt(rest) / jnp.sqrt(bar_now),
            jnp.sqrt(bar_next) - lift * jnp.sqrt(bar_now),
            lift - 1.0,
            jnp.sqrt((1.0 - bar_next) / rest * (1.0 - bar_now / bar_next)),
        ]
        for i, coef in enumerate(coefs):
            coef_v[i] = coef
        angles = level_now.astype(F32) * freq_ref[...]
        around = jnp.concatenate([jnp.cos(angles), jnp.sin(angles)], axis=1).astype(BF16)
        loads[4].wait()
        modulation_v[...] = jnp.dot(around, wemb[...], preferred_element_type=F32)

    def modulations(low):
        cut = pl.ds(low, BLOCK)
        return jnp.concatenate(
            [modulation_v[t : t + 1, cut] for t in range(plane)], axis=0
        ).reshape(plane, 1, BLOCK)

    def drifts(n, j, eps):
        result = []
        for t in range(plane):
            state = start_v[j] if n == 0 else state_v[j, t]
            coef = [coef_v[i][t : t + 1, :1] for i in range(5)]
            clean = jnp.clip(state * coef[0] - eps[t] * coef[1], -1.0, 1.0)
            result.append(coef[2] * clean + coef[3] * state + coef[4] * noise_all[t, j])
        return result

    def launch(n, j):
        @pl.when(z == 0)
        def _():
            for q in range(PIECES):
                chain_copy(n, j, q).start()

    def forward(n, j, q):
        @pl.when(z > 0)
        def _():
            cut = pl.ds(q * depth, depth)
            chain_copy(n, j, q).wait_recv()
            chain_tx[n, j, cut] = chain_tx[n, j, cut] + chain_rx[n, j, cut]

            @pl.when(z < rows - 1)
            def _():
                chain_copy(n, j, q).start()

    def denoise(entries, norms, hook, outer):
        images, times = entries[0].shape[:2]
        count = images * plane
        ones = []
        for i, (shifted, mean, spread) in enumerate(norms):
            scale, shift = modulations(i * BLOCK), modulations(channels + i * BLOCK)
            gain = spread * (0.5 + 0.5 * scale[None])
            ones.append(flatten(silu_of_half(shifted * gain + (0.5 * shift[None] - mean * gain))))
        hook(0)
        twos = activate(shape_images(project(ones, w1, outer), count))
        hook(1)
        blocks = []
        for entry, extra in zip(entries, project(twos, w2, outer)):
            total = entry + extra.reshape(images, plane, patches, BLOCK)
            blocks.append(total.reshape(count, patches, BLOCK))
        threes = activate(blocks)
        hook(2)
        eps = jnp.concatenate(project(threes, wout, outer), axis=1)
        hook(3)
        return eps.reshape(images, plane, patches, features)

    def entrance(flat, images, times, outer):
        count = images * times
        blocks = shape_images(project(cut_columns(flat), win, outer), count)
        entries = [block.reshape(images, times, patches, BLOCK) for block in blocks]
        norms = []
        for block in blocks:
            shifted, mean, spread = centered(block)
            stats = (value.reshape(images, times, 1, BLOCK) for value in (mean, spread))
            norms.append((shifted.reshape(images, times, patches, BLOCK), *stats))
        return entries, norms

    def finish_first(j, eps):
        if j == 0:
            loads[3].wait()
        for r in range(1, plane):
            slot = mate(r)[0]
            noise_copy(j, r, slot).wait_recv()
        parts = drifts(0, j, eps)
        running = parts[0]
        for t in range(1, plane):
            part_v[j, t] = running
            running = running + parts[t]
        chain_tx[0, j] = running
        launch(0, j)

    def second(j, hook):
        state_v[j, 0] = start_v[j] + chain_rx[0, j]
        for t in range(1, plane):
            state_v[j, t] = start_v[j] + (chain_rx[0, j] + part_v[j, t])
        flat = state_v[j].reshape(plane * patches, features).astype(BF16)
        eps = denoise(*entrance(flat, 1, plane, OUTER_TWO), hook, OUTER_TWO)[0]
        parts = drifts(1, j, eps)
        running = parts[0]
        origin = start_v[j]
        out_tx[j, 0] = origin + running
        for t in range(1, plane):
            running = running + parts[t]
            out_tx[j, t] = origin + running
        chain_tx[1, j] = running
        launch(1, j)
        for q in range(PIECES):
            forward(1, j, q)
            cut = pl.ds(q * depth, depth)
            for t in range(plane):
                out_tx[j, t, cut] = out_tx[j, t, cut] + chain_rx[1, j, cut]
            for r in range(1, plane):
                out_copy(j, r, p, q).start()
        out_v[first + j] = out_tx[j, p]

    for i in (1, 2, 12):
        loads[i].wait()
    flat = start_v[...].reshape(own * patches, features).astype(BF16)
    entries, norms = entrance(flat, own, 1, OUTER_ONE)
    for i in (5, 6, 7):
        loads[i].wait()
    set_levels()

    def idle(stage):
        pass

    eps = denoise(entries, norms, idle, OUTER_ONE)
    for j in range(1, own):
        eps_v[j - 1] = eps[j]
    finish_first(0, eps[0])

    for j in range(1, own):

        def relay(stage):
            if stage == 2:
                forward(0, j, 0)
            if stage == 3:
                for q in range(1, PIECES // 2 + 1):
                    forward(0, j, q)

        if j == 1:
            for q in range(PIECES):
                forward(0, 0, q)

        @pl.when(z > 0)
        def _():
            finish_first(j, eps_v[j - 1])

        second(j - 1, relay)

        @pl.when(z == 0)
        def _():
            finish_first(j, eps_v[j - 1])

        for q in range(PIECES // 2 + 1, PIECES):
            forward(0, j, q)

    second(own - 1, idle)

    for r in range(1, plane):
        slot = mate(r)[0]
        for j in range(own):
            for q in range(PIECES):
                out_copy(j, r, slot, q).wait_recv()

    for r in range(1, plane):
        gap_copy(r, p).wait_send()
        for j in range(own):
            noise_copy(j, r, p).wait_send()
            for q in range(PIECES):
                out_copy(j, r, p, q).wait_send()

    @pl.when(z < rows - 1)
    def _():
        base_copy().wait_send()
        for n in range(ITERS):
            for j in range(own):
                for q in range(PIECES):
                    chain_copy(n, j, q).wait_send()


def shards(
    steps,
    inner,
    start_state,
    noise_draws,
    step_gaps,
    window_start,
    input_weight,
    embed_weight,
    first_weight,
    second_weight,
    output_weight,
):
    batch, patches, features = start_state.shape
    channels = input_weight.shape[1]
    columns = 2 if steps % 2 == 0 else 1
    plane = columns * inner
    own = batch // plane
    cfg = (steps, inner, columns, own, patches, features, channels)
    image = (patches, features)
    table = jnp.asarray(noise_table())
    freq = jnp.asarray(frequencies(embed_weight.shape[0] // 2))
    matrix = jnp.asarray(group_matrix(channels, patches)).astype(BF16)
    vmem = pl.BlockSpec(memory_space=pltpu.VMEM)
    anywhere = pl.BlockSpec(memory_space=pltpu.HBM)
    dma = pltpu.SemaphoreType.DMA
    out = pl.pallas_call(
        functools.partial(kernel, cfg),
        out_shape=pltpu.VMEM((batch,) + image, F32),
        in_specs=[anywhere] * 12,
        out_specs=vmem,
        scratch_shapes=[
            pltpu.SMEM((1,), jnp.int32),
            pltpu.SMEM((1,), jnp.int32),
            pltpu.VMEM(table.shape, F32),
            pltpu.VMEM(freq.shape, F32),
            pltpu.VMEM(matrix.shape, BF16),
            pltpu.VMEM((own,) + image, F32),
            pltpu.VMEM((batch,) + image, F32),
            pltpu.VMEM((plane, own) + image, F32),
            pltpu.VMEM(input_weight.shape, BF16),
            pltpu.VMEM(embed_weight.shape, BF16),
            pltpu.VMEM(first_weight.shape, BF16),
            pltpu.VMEM(second_weight.shape, BF16),
            pltpu.VMEM(output_weight.shape, BF16),
            pltpu.VMEM((8, LANES), jnp.int32),
            pltpu.VMEM((plane, 8, LANES), jnp.int32),
            pltpu.VMEM((8, LANES), jnp.int32),
            pltpu.VMEM((8, LANES), jnp.int32),
            pltpu.VMEM((8, 2 * channels), F32),
            pltpu.VMEM((5, 8, LANES), F32),
            pltpu.VMEM((own, plane) + image, F32),
            pltpu.VMEM((own, plane) + image, F32),
            pltpu.VMEM((ITERS, own) + image, F32),
            pltpu.VMEM((ITERS, own) + image, F32),
            pltpu.VMEM((own, plane) + image, F32),
            pltpu.VMEM((max(own - 1, 1), plane) + image, F32),
            dma((13,)),
            dma((plane,)),
            dma((plane,)),
            dma((2,)),
            dma((own, plane)),
            dma((plane, own)),
            dma((ITERS, own, PIECES)),
            dma((ITERS, own, PIECES)),
            dma((own, plane, PIECES)),
            dma((plane, own, PIECES)),
        ],
        compiler_params=pltpu.CompilerParams(
            collective_id=0, has_side_effects=True, vmem_limit_bytes=56 * 1024 * 1024
        ),
    )(
        step_gaps,
        window_start,
        table,
        freq,
        matrix,
        start_state,
        noise_draws.reshape((batch,) + image),
        input_weight,
        embed_weight,
        first_weight,
        second_weight,
        output_weight,
    )
    return out.reshape((1,) + start_state.shape)


def solution(mesh):
    steps, inner = mesh.shape["steps"], mesh.shape["inner"]
    return jax.shard_map(
        functools.partial(shards, steps, inner),
        mesh=mesh,
        in_specs=(
            P("groups", None, None),
            P(("groups", "steps", "inner"), None, None, None),
            P(("groups", "steps", "inner")),
            P("groups"),
            P(),
            P(),
            P(),
            P(),
            P(),
        ),
        out_specs=P(("groups", "steps", "inner"), None, None, None),
        check_vma=False,
    )
```

```python
import functools
import math

import jax
import jax.numpy as jnp
import numpy as np
from jax import lax
from jax.experimental import pallas as pl
from jax.experimental.pallas import tpu as pltpu
from jax.sharding import PartitionSpec as P

GROUPS = 32
PIECES = 4
OUTER_ONE = False
OUTER_TWO = False
ITERS = 2
TRAIN_STEPS = 1000
LANES = 128
BLOCK = 256
MESH = pl.DeviceIdType.MESH
F32 = jnp.float32
BF16 = jnp.bfloat16


def noise_table():
    levels = np.arange(TRAIN_STEPS, dtype=np.float32)
    beta = (0.0001 + (0.02 - 0.0001) * levels / (TRAIN_STEPS - 1)).astype(np.float32)
    bars = np.exp(np.cumsum(np.log1p(-beta.astype(np.float64)))).astype(np.float32)
    padded = np.zeros((-(-TRAIN_STEPS // (8 * LANES)) * 8 * LANES,), np.float32)
    padded[:TRAIN_STEPS] = bars
    return padded.reshape(-1, LANES)


def frequencies(count):
    powers = -math.log(10000.0) * np.arange(count, dtype=np.float32) / count
    return np.exp(powers.astype(np.float32)).astype(np.float32)[None, :]


def group_matrix(channels, rows):
    width = channels // GROUPS
    place = np.arange(BLOCK) // width
    same = (place[:, None] == place[None, :]).astype(np.float32)
    return same / (width * rows)


def silu_of_half(half):
    return half + half * jnp.tanh(half)


def kernel(
    cfg,
    gap_hbm,
    start_level_hbm,
    table_hbm,
    freq_hbm,
    group_hbm,
    start_hbm,
    noise_hbm,
    win_hbm,
    wemb_hbm,
    w1_hbm,
    w2_hbm,
    wout_hbm,
    out_v,
    gap_ref,
    start_level_ref,
    table_ref,
    freq_ref,
    group_ref,
    start_v,
    noise_v,
    noise_all,
    win,
    wemb,
    w1,
    w2,
    wout,
    gap_send,
    gap_all,
    base_rx,
    base_tx,
    modulation_v,
    coef_v,
    part_v,
    state_v,
    chain_rx,
    chain_tx,
    out_tx,
    eps_v,
    pair_rx,
    sum_tx,
    sum_rx,
    raw_tx,
    raw_rx,
    late_v,
    load_sem,
    gap_send_sem,
    gap_recv_sem,
    base_sem,
    noise_send,
    noise_recv,
    chain_send,
    chain_recv,
    out_send,
    out_recv,
    late_send,
    late_recv,
):
    steps, inner, columns, own, patches, features, channels = cfg
    rows = steps // columns
    plane = columns * inner
    s = lax.axis_index("steps")
    h = lax.axis_index("inner")
    z = s // columns
    y = lax.rem(s, columns)
    p = y * inner + h
    first = p * own
    late = own - 1 if own > 1 and columns == 2 and inner == 2 else None
    partner, across, other = p + 1 - 2 * h, (1 - y) * inner + h, (1 - y) * inner

    def load(i, src, dst):
        return pltpu.make_async_copy(src, dst, load_sem.at[i])

    loads = [
        load(0, noise_hbm, noise_v),
        load(1, start_hbm.at[pl.ds(first, own)], start_v),
        load(2, win_hbm, win),
        load(3, noise_hbm.at[pl.ds(first, own)], noise_all.at[p]),
        load(4, wemb_hbm, wemb),
        load(5, w1_hbm, w1),
        load(6, w2_hbm, w2),
        load(7, wout_hbm, wout),
        load(8, gap_hbm, gap_ref),
        load(9, start_level_hbm, start_level_ref),
        load(10, table_hbm, table_ref),
        load(11, freq_hbm, freq_ref),
        load(12, group_hbm, group_ref),
    ]
    def mate(r):
        q = lax.rem(p + r, plane)
        return q, {"steps": z * columns + q // inner, "inner": lax.rem(q, inner)}

    below, above = {"steps": s - columns}, {"steps": s + columns}

    barrier = pltpu.get_barrier_semaphore()
    for r in range(1, plane):
        pl.semaphore_signal(barrier, inc=1, device_id=mate(r)[1], device_id_type=MESH)

    @pl.when(z > 0)
    def _():
        pl.semaphore_signal(barrier, inc=1, device_id=below, device_id_type=MESH)

    for i in (8, 0, 9, 10, 11, 1, 2, 12, 3, 4, 5, 6, 7):
        loads[i].start()

    loads[8].wait()
    gap_send[...] = jnp.zeros_like(gap_send) + gap_ref[0]
    gap_all[p] = jnp.zeros_like(gap_send) + gap_ref[0]

    @pl.when(z == 0)
    def _():
        base_rx[...] = jnp.zeros_like(base_rx)
        chain_rx[...] = jnp.zeros_like(chain_rx)

    neighbours = (2 * rows - 2 - z) // rows
    pl.semaphore_wait(barrier, plane - 1 + neighbours)

    def gap_copy(r, slot):
        return pltpu.make_async_remote_copy(
            src_ref=gap_send,
            dst_ref=gap_all.at[slot],
            send_sem=gap_send_sem.at[r],
            recv_sem=gap_recv_sem.at[slot],
            device_id=mate(r)[1],
            device_id_type=MESH,
        )

    def base_copy():
        return pltpu.make_async_remote_copy(
            src_ref=base_tx,
            dst_ref=base_rx,
            send_sem=base_sem.at[0],
            recv_sem=base_sem.at[1],
            device_id=above,
            device_id_type=MESH,
        )

    def noise_copy(j, r, slot):
        q, device = mate(r)
        return pltpu.make_async_remote_copy(
            src_ref=noise_v.at[q * own + j],
            dst_ref=noise_all.at[slot, j],
            send_sem=noise_send.at[j, r],
            recv_sem=noise_recv.at[slot, j],
            device_id=device,
            device_id_type=MESH,
        )

    depth = patches // PIECES

    def out_copy(j, r, slot, piece):
        q, device = mate(r)
        cut = pl.ds(piece * depth, depth)
        return pltpu.make_async_remote_copy(
            src_ref=out_tx.at[j, q, cut],
            dst_ref=out_v.at[slot * own + j, cut],
            send_sem=out_send.at[j, r, piece],
            recv_sem=out_recv.at[slot, j, piece],
            device_id=device,
            device_id_type=MESH,
        )

    def chain_copy(n, j, q):
        cut = pl.ds(q * depth, depth)
        return pltpu.make_async_remote_copy(
            src_ref=chain_tx.at[n, j, cut],
            dst_ref=chain_rx.at[n, j, cut],
            send_sem=chain_send.at[n, j, q],
            recv_sem=chain_recv.at[n, j, q],
            device_id=above,
            device_id_type=MESH,
        )

    def late_copy(i, src, dst, device):
        return pltpu.make_async_remote_copy(
            src_ref=src,
            dst_ref=dst,
            send_sem=late_send.at[i],
            recv_sem=late_recv.at[i],
            device_id=device,
            device_id_type=MESH,
        )

    def late_move(i, slot):
        beside, over = {"inner": 1 - h}, {"steps": z * columns + 1 - y}
        if i == 0:
            return late_copy(0, noise_v.at[(other + 1 - h) * own + late], pair_rx, beside)
        if i == 1:
            return late_copy(
                1, noise_v.at[partner * own + late], noise_all.at[slot, late], beside
            )
        return late_copy(i, *((sum_tx, sum_rx) if i == 2 else (raw_tx, raw_rx)), over)

    plain = [j for j in range(own) if j != late]
    for r in range(1, plane):
        gap_copy(r, p).start()
    loads[0].wait()
    for j in plain:
        for r in range(1, plane):
            noise_copy(j, r, p).start()
    if late is not None:
        for i in (0, 1):
            late_move(i, p).start()

    def cut_columns(value):
        return [value[..., i : i + BLOCK] for i in range(0, value.shape[-1], BLOCK)]

    def pack(partial):
        row = lax.broadcasted_iota(jnp.int32, (8, BLOCK), 0)
        top, late = row < 4, lax.rem(row, 4) >= 2
        packed = []
        for i in range(0, partial.shape[0], 4):
            a, b, c, d = (partial[i + k] for k in range(4))
            ab = jnp.where(top, a, b) + pltpu.roll(jnp.where(top, b, a), 4, 0)
            cd = jnp.where(top, c, d) + pltpu.roll(jnp.where(top, d, c), 4, 0)
            four = jnp.where(late, ab + pltpu.roll(ab, 2, 0), cd + pltpu.roll(cd, 6, 0))
            packed.append(four + pltpu.roll(four, 1, 0))
        return packed

    def group_averages(partials):
        size = partials[0].shape[0]
        whole = size % 4 == 0
        rows = []
        for partial in partials:
            rows.extend(pack(partial) if whole else [partial.reshape(size * 8, BLOCK)])
        rows = jnp.concatenate(rows, axis=0)
        high = rows.astype(BF16).astype(F32)
        rest = rows - high
        middle = rest.astype(BF16).astype(F32)
        parts = jnp.concatenate([rest - middle, middle, high], axis=0).astype(BF16)
        summed = jnp.dot(parts, group_ref[...], preferred_element_type=F32)
        summed = jnp.sum(summed.reshape(3, len(partials), -1, BLOCK), axis=0)
        if not whole:
            summed = summed.reshape(len(partials), size, 8, BLOCK)
            return list(jnp.sum(summed, axis=2, keepdims=True))
        places = [i // 4 * 8 + (3, 7, 1, 5)[i % 4] for i in range(size)]
        return [jnp.stack([block[r : r + 1] for r in places], axis=0) for block in summed]

    def row_sums(value):
        size = value.shape[0]
        return jnp.sum(value.reshape(size, patches // 8, 8, BLOCK), axis=1)

    def pivots(block):
        rows = block[:, 0, :]
        lane = lax.broadcasted_iota(jnp.int32, (rows.shape[0], LANES), 1)
        lead = lane - lax.rem(lane, channels // GROUPS)
        halves = [
            jnp.take_along_axis(rows[:, i : i + LANES], lead, axis=1)
            for i in range(0, BLOCK, LANES)
        ]
        return jnp.concatenate(halves, axis=1)[:, None, :]

    def centered(block):
        shifted = block - pivots(block)
        mean, square = group_averages([row_sums(shifted), row_sums(shifted * shifted)])
        return shifted, mean, lax.rsqrt(jnp.maximum(square - mean * mean, 0.0) + 1e-05)

    def project(acts, weight, outer=True):
        sums = [None] * (weight.shape[1] // BLOCK)
        pairs = [(k, n) for k in range(len(acts)) for n in range(len(sums))]
        if not outer:
            pairs = [(k, n) for n in range(len(sums)) for k in range(len(acts))]
        for k, n in pairs:
            tile = weight[pl.ds(k * BLOCK, BLOCK), pl.ds(n * BLOCK, BLOCK)]
            part = jnp.dot(acts[k], tile, preferred_element_type=F32)
            sums[n] = part if sums[n] is None else sums[n] + part
        return sums

    def shape_images(blocks, size):
        return [block.reshape(size, patches, BLOCK) for block in blocks]

    def flatten(value):
        return value.reshape(-1, BLOCK).astype(BF16)

    def activate(blocks):
        result = []
        for block in blocks:
            shifted, mean, spread = centered(block)
            gain = 0.5 * spread
            result.append(flatten(silu_of_half(shifted * gain - mean * gain)))
        return result

    def set_levels():
        for r in range(1, plane):
            slot = mate(r)[0]
            gap_copy(r, slot).wait_recv()

        @pl.when(z > 0)
        def _():
            base_copy().wait_recv()

        gaps = [gap_all[t] for t in range(plane)]
        base = base_rx[...]
        total = base
        for gap in gaps:
            total = total + gap
        base_tx[...] = total

        @pl.when(z < rows - 1)
        def _():
            base_copy().start()

        for i in (9, 10, 11):
            loads[i].wait()
        table = table_ref[...]
        tall = lax.broadcasted_iota(jnp.int32, table.shape, 0)
        places = tall * LANES + lax.broadcasted_iota(jnp.int32, table.shape, 1)
        level = start_level_ref[0] - base
        levels = [level]
        for gap in gaps:
            level = level - gap
            levels.append(level)

        def lookup(level):
            found = jnp.where(places == level[:1, :1], table, 0.0)
            return jnp.sum(jnp.sum(found, axis=0, keepdims=True), axis=1, keepdims=True)

        bars = [lookup(level) for level in levels]
        bar_now, bar_next = jnp.ones(table.shape, F32), jnp.ones(table.shape, F32)
        level_now = levels[0]
        for t in range(plane):
            bar_now = jnp.where(tall == t, bars[t], bar_now)
            bar_next = jnp.where(tall == t, bars[t + 1], bar_next)
            level_now = jnp.where(tall == t, levels[t], level_now)
        rest = 1.0 - bar_now
        lift = (1.0 - bar_next) * jnp.sqrt(bar_now / (bar_next * rest)) / jnp.sqrt(rest)
        coefs = [
            1.0 / jnp.sqrt(bar_now),
            jnp.sqrt(rest) / jnp.sqrt(bar_now),
            jnp.sqrt(bar_next) - lift * jnp.sqrt(bar_now),
            lift - 1.0,
            jnp.sqrt((1.0 - bar_next) / rest * (1.0 - bar_now / bar_next)),
        ]
        for i, coef in enumerate(coefs):
            coef_v[i] = coef
        angles = level_now.astype(F32) * freq_ref[...]
        around = jnp.concatenate([jnp.cos(angles), jnp.sin(angles)], axis=1).astype(BF16)
        loads[4].wait()
        modulation_v[...] = jnp.dot(around, wemb[...], preferred_element_type=F32)

    def modulations(low):
        cut = pl.ds(low, BLOCK)
        return jnp.concatenate(
            [modulation_v[t : t + 1, cut] for t in range(plane)], axis=0
        ).reshape(plane, 1, BLOCK)

    def noise_of(n, j, t):
        if j != late:
            return coef_v[4][t : t + 1, :1] * noise_all[t, j]
        return late_v[t] if n else None

    def drifts(n, j, eps):
        result = []
        for t in range(plane):
            state = start_v[j] if n == 0 else state_v[j, t]
            coef = [coef_v[i][t : t + 1, :1] for i in range(4)]
            clean = jnp.clip(state * coef[0] - eps[t] * coef[1], -1.0, 1.0)
            drift = coef[2] * clean + coef[3] * state
            noise = noise_of(n, j, t)
            result.append(drift if noise is None else drift + noise)
        return result

    def weight(slot):
        return coef_v[4, pl.ds(slot, 1), :1]

    def blend():
        late_move(0, p).wait_recv()
        mine, theirs = noise_v[across * own + late], pair_rx[...]
        sum_tx[...] = weight(p) * mine + weight(partner) * theirs
        raw_tx[...] = jnp.where(h == 0, mine, theirs)
        for i in (2, 3):
            late_move(i, p).start()

    def launch(n, j):
        @pl.when(z == 0)
        def _():
            for q in range(PIECES):
                chain_copy(n, j, q).start()

    def forward(n, j, q):
        @pl.when(z > 0)
        def _():
            cut = pl.ds(q * depth, depth)
            chain_copy(n, j, q).wait_recv()
            chain_tx[n, j, cut] = chain_tx[n, j, cut] + chain_rx[n, j, cut]

            @pl.when(z < rows - 1)
            def _():
                chain_copy(n, j, q).start()

    def denoise(entries, norms, hook, outer):
        images, times = entries[0].shape[:2]
        count = images * plane
        ones = []
        for i, (shifted, mean, spread) in enumerate(norms):
            scale, shift = modulations(i * BLOCK), modulations(channels + i * BLOCK)
            gain = spread * (0.5 + 0.5 * scale[None])
            ones.append(flatten(silu_of_half(shifted * gain + (0.5 * shift[None] - mean * gain))))
        hook(0)
        twos = activate(shape_images(project(ones, w1, outer), count))
        hook(1)
        blocks = []
        for entry, extra in zip(entries, project(twos, w2, outer)):
            total = entry + extra.reshape(images, plane, patches, BLOCK)
            blocks.append(total.reshape(count, patches, BLOCK))
        threes = activate(blocks)
        hook(2)
        eps = jnp.concatenate(project(threes, wout, outer), axis=1)
        hook(3)
        return eps.reshape(images, plane, patches, features)

    def entrance(flat, images, times, outer):
        count = images * times
        blocks = shape_images(project(cut_columns(flat), win, outer), count)
        entries = [block.reshape(images, times, patches, BLOCK) for block in blocks]
        norms = []
        for block in blocks:
            shifted, mean, spread = centered(block)
            stats = (value.reshape(images, times, 1, BLOCK) for value in (mean, spread))
            norms.append((shifted.reshape(images, times, patches, BLOCK), *stats))
        return entries, norms

    def finish_first(j, eps):
        if j == 0:
            loads[3].wait()
        if j != late:
            for r in range(1, plane):
                slot = mate(r)[0]
                noise_copy(j, r, slot).wait_recv()
        parts = drifts(0, j, eps)
        running = parts[0]
        for t in range(1, plane):
            part_v[j, t] = running
            running = running + parts[t]
        if j == late:
            for i in (1, 2):
                late_move(i, partner).wait_recv()
            near = y * inner
            for i in range(inner):
                late_v[near + i] = weight(near + i) * noise_all[near + i, late]
            running = running + (late_v[near] + late_v[near + 1] + sum_rx[...])
        chain_tx[0, j] = running
        launch(0, j)

    def finish_late():
        late_move(3, partner).wait_recv()
        lead = weight(other) * raw_rx[...]
        late_v[other] = lead
        late_v[other + 1] = sum_rx[...] - lead
        running = late_v[0]
        for t in range(1, plane):
            part_v[late, t] = part_v[late, t] + running
            running = running + late_v[t]

    def second(j, hook):
        if j == late:
            finish_late()
        state_v[j, 0] = start_v[j] + chain_rx[0, j]
        for t in range(1, plane):
            state_v[j, t] = start_v[j] + (chain_rx[0, j] + part_v[j, t])
        flat = state_v[j].reshape(plane * patches, features).astype(BF16)
        eps = denoise(*entrance(flat, 1, plane, OUTER_TWO), hook, OUTER_TWO)[0]
        parts = drifts(1, j, eps)
        running = parts[0]
        origin = start_v[j]
        out_tx[j, 0] = origin + running
        for t in range(1, plane):
            running = running + parts[t]
            out_tx[j, t] = origin + running
        chain_tx[1, j] = running
        launch(1, j)
        for q in range(PIECES):
            forward(1, j, q)
            cut = pl.ds(q * depth, depth)
            for t in range(plane):
                out_tx[j, t, cut] = out_tx[j, t, cut] + chain_rx[1, j, cut]
            for r in range(1, plane):
                out_copy(j, r, p, q).start()
        out_v[first + j] = out_tx[j, p]

    for i in (1, 2, 12):
        loads[i].wait()
    flat = start_v[...].reshape(own * patches, features).astype(BF16)
    entries, norms = entrance(flat, own, 1, OUTER_ONE)
    for i in (5, 6, 7):
        loads[i].wait()
    set_levels()

    def idle(stage):
        pass

    if late is not None:
        blend()
    eps = denoise(entries, norms, idle, OUTER_ONE)
    for j in range(1, own):
        eps_v[j - 1] = eps[j]
    finish_first(0, eps[0])

    for q in range(PIECES):
        forward(0, 0, q)
    for j in range(1, own):

        @pl.when(z > 0)
        def _():
            finish_first(j, eps_v[j - 1])

        def relay(stage):
            if stage == 2:

                @pl.when(z == 0)
                def _():
                    finish_first(j, eps_v[j - 1])

            if stage < PIECES:
                forward(0, j, stage)

        second(j - 1, relay)
        for q in range(4, PIECES):
            forward(0, j, q)

    second(own - 1, idle)

    for r in range(1, plane):
        slot = mate(r)[0]
        for j in range(own):
            for q in range(PIECES):
                out_copy(j, r, slot, q).wait_recv()

    for r in range(1, plane):
        gap_copy(r, p).wait_send()
        for j in plain:
            noise_copy(j, r, p).wait_send()
        for j in range(own):
            for q in range(PIECES):
                out_copy(j, r, p, q).wait_send()
    if late is not None:
        for i in range(4):
            late_move(i, p).wait_send()

    @pl.when(z < rows - 1)
    def _():
        base_copy().wait_send()
        for n in range(ITERS):
            for j in range(own):
                for q in range(PIECES):
                    chain_copy(n, j, q).wait_send()


def shards(
    steps,
    inner,
    start_state,
    noise_draws,
    step_gaps,
    window_start,
    input_weight,
    embed_weight,
    first_weight,
    second_weight,
    output_weight,
):
    batch, patches, features = start_state.shape
    channels = input_weight.shape[1]
    columns = 2 if steps % 2 == 0 else 1
    plane = columns * inner
    own = batch // plane
    cfg = (steps, inner, columns, own, patches, features, channels)
    image = (patches, features)
    table = jnp.asarray(noise_table())
    freq = jnp.asarray(frequencies(embed_weight.shape[0] // 2))
    matrix = jnp.asarray(group_matrix(channels, patches)).astype(BF16)
    vmem = pl.BlockSpec(memory_space=pltpu.VMEM)
    anywhere = pl.BlockSpec(memory_space=pltpu.HBM)
    dma = pltpu.SemaphoreType.DMA
    out = pl.pallas_call(
        functools.partial(kernel, cfg),
        out_shape=pltpu.VMEM((batch,) + image, F32),
        in_specs=[anywhere] * 12,
        out_specs=vmem,
        scratch_shapes=[
            pltpu.SMEM((1,), jnp.int32),
            pltpu.SMEM((1,), jnp.int32),
            pltpu.VMEM(table.shape, F32),
            pltpu.VMEM(freq.shape, F32),
            pltpu.VMEM(matrix.shape, BF16),
            pltpu.VMEM((own,) + image, F32),
            pltpu.VMEM((batch,) + image, F32),
            pltpu.VMEM((plane, own) + image, F32),
            pltpu.VMEM(input_weight.shape, BF16),
            pltpu.VMEM(embed_weight.shape, BF16),
            pltpu.VMEM(first_weight.shape, BF16),
            pltpu.VMEM(second_weight.shape, BF16),
            pltpu.VMEM(output_weight.shape, BF16),
            pltpu.VMEM((8, LANES), jnp.int32),
            pltpu.VMEM((plane, 8, LANES), jnp.int32),
            pltpu.VMEM((8, LANES), jnp.int32),
            pltpu.VMEM((8, LANES), jnp.int32),
            pltpu.VMEM((8, 2 * channels), F32),
            pltpu.VMEM((5, 8, LANES), F32),
            pltpu.VMEM((own, plane) + image, F32),
            pltpu.VMEM((own, plane) + image, F32),
            pltpu.VMEM((ITERS, own) + image, F32),
            pltpu.VMEM((ITERS, own) + image, F32),
            pltpu.VMEM((own, plane) + image, F32),
            pltpu.VMEM((max(own - 1, 1), plane) + image, F32),
        ]
        + [pltpu.VMEM(image, F32)] * 5
        + [
            pltpu.VMEM((plane,) + image, F32),
            dma((13,)),
            dma((plane,)),
            dma((plane,)),
            dma((2,)),
            dma((own, plane)),
            dma((plane, own)),
            dma((ITERS, own, PIECES)),
            dma((ITERS, own, PIECES)),
            dma((own, plane, PIECES)),
            dma((plane, own, PIECES)),
            dma((4,)),
            dma((4,)),
        ],
        compiler_params=pltpu.CompilerParams(
            collective_id=0, has_side_effects=True, vmem_limit_bytes=56 * 1024 * 1024
        ),
    )(
        step_gaps,
        window_start,
        table,
        freq,
        matrix,
        start_state,
        noise_draws.reshape((batch,) + image),
        input_weight,
        embed_weight,
        first_weight,
        second_weight,
        output_weight,
    )
    return out.reshape((1,) + start_state.shape)


def solution(mesh):
    steps, inner = mesh.shape["steps"], mesh.shape["inner"]
    return jax.shard_map(
        functools.partial(shards, steps, inner),
        mesh=mesh,
        in_specs=(
            P("groups", None, None),
            P(("groups", "steps", "inner"), None, None, None),
            P(("groups", "steps", "inner")),
            P("groups"),
            P(),
            P(),
            P(),
            P(),
            P(),
        ),
        out_specs=P(("groups", "steps", "inner"), None, None, None),
        check_vma=False,
    )
```

```python
import functools
import math

import jax
import jax.numpy as jnp
import numpy as np
from jax import lax
from jax.experimental import pallas as pl
from jax.experimental.pallas import tpu as pltpu
from jax.sharding import PartitionSpec as P

GROUPS = 32
PIECES = 4
LATE_STAGE = 3
RELAY = {1: (0, 1), 3: (2, 3)}
OUTER_ONE = False
OUTER_TWO = False
ITERS = 2
TRAIN_STEPS = 1000
LANES = 128
BLOCK = 256
MESH = pl.DeviceIdType.MESH
F32 = jnp.float32
BF16 = jnp.bfloat16


def noise_table():
    levels = np.arange(TRAIN_STEPS, dtype=np.float32)
    beta = (0.0001 + (0.02 - 0.0001) * levels / (TRAIN_STEPS - 1)).astype(np.float32)
    bars = np.exp(np.cumsum(np.log1p(-beta.astype(np.float64)))).astype(np.float32)
    padded = np.zeros((-(-TRAIN_STEPS // (8 * LANES)) * 8 * LANES,), np.float32)
    padded[:TRAIN_STEPS] = bars
    return padded.reshape(-1, LANES)


def frequencies(count):
    powers = -math.log(10000.0) * np.arange(count, dtype=np.float32) / count
    return np.exp(powers.astype(np.float32)).astype(np.float32)[None, :]


def group_matrix(channels, rows):
    width = channels // GROUPS
    place = np.arange(BLOCK) // width
    same = (place[:, None] == place[None, :]).astype(np.float32)
    return same / (width * rows)


def silu_of_half(half):
    return half + half * jnp.tanh(half)


def kernel(
    cfg,
    gap_ref,
    start_level_ref,
    table_hbm,
    freq_hbm,
    group_hbm,
    start_hbm,
    noise_hbm,
    win_hbm,
    wemb_hbm,
    w1_hbm,
    w2_hbm,
    wout_hbm,
    out_v,
    table_ref,
    freq_ref,
    group_ref,
    start_v,
    noise_v,
    noise_all,
    win,
    wemb,
    w1,
    w2,
    wout,
    gap_send,
    gap_all,
    base_rx,
    base_tx,
    modulation_v,
    coef_v,
    part_v,
    state_v,
    chain_rx,
    chain_tx,
    out_tx,
    eps_v,
    pair_rx,
    sum_tx,
    sum_rx,
    raw_tx,
    raw_rx,
    late_v,
    load_sem,
    gap_send_sem,
    gap_recv_sem,
    base_sem,
    noise_send,
    noise_recv,
    chain_send,
    chain_recv,
    out_send,
    out_recv,
    late_send,
    late_recv,
):
    steps, inner, columns, own, patches, features, channels = cfg
    rows = steps // columns
    plane = columns * inner
    s = lax.axis_index("steps")
    h = lax.axis_index("inner")
    z = s // columns
    y = lax.rem(s, columns)
    p = y * inner + h
    first = p * own
    late = own - 1 if own > 1 and columns == 2 and inner == 2 else None
    partner, across, other = p + 1 - 2 * h, (1 - y) * inner + h, (1 - y) * inner

    def load(i, src, dst):
        return pltpu.make_async_copy(src, dst, load_sem.at[i])

    loads = [
        load(0, noise_hbm, noise_v),
        load(1, start_hbm.at[pl.ds(first, own)], start_v),
        load(2, win_hbm, win),
        load(3, noise_hbm.at[pl.ds(first, own)], noise_all.at[p]),
        load(4, wemb_hbm, wemb),
        load(5, w1_hbm, w1),
        load(6, w2_hbm, w2),
        load(7, wout_hbm, wout),
        load(8, table_hbm, table_ref),
        load(9, freq_hbm, freq_ref),
        load(10, group_hbm, group_ref),
    ]
    def mate(r):
        q = lax.rem(p + r, plane)
        return q, {"steps": z * columns + q // inner, "inner": lax.rem(q, inner)}

    below, above = {"steps": s - columns}, {"steps": s + columns}

    barrier = pltpu.get_barrier_semaphore()
    for r in range(1, plane):
        pl.semaphore_signal(barrier, inc=1, device_id=mate(r)[1], device_id_type=MESH)

    @pl.when(z > 0)
    def _():
        pl.semaphore_signal(barrier, inc=1, device_id=below, device_id_type=MESH)

    for i in (0, 1, 2, 8, 9, 10, 3, 4, 5, 6, 7):
        loads[i].start()

    gap_send[...] = jnp.zeros_like(gap_send) + gap_ref[0]
    gap_all[p] = jnp.zeros_like(gap_send) + gap_ref[0]

    @pl.when(z == 0)
    def _():
        base_rx[...] = jnp.zeros_like(base_rx)
        chain_rx[...] = jnp.zeros_like(chain_rx)

    neighbours = (2 * rows - 2 - z) // rows
    pl.semaphore_wait(barrier, plane - 1 + neighbours)

    def gap_copy(r, slot):
        return pltpu.make_async_remote_copy(
            src_ref=gap_send,
            dst_ref=gap_all.at[slot],
            send_sem=gap_send_sem.at[r],
            recv_sem=gap_recv_sem.at[slot],
            device_id=mate(r)[1],
            device_id_type=MESH,
        )

    def base_copy():
        return pltpu.make_async_remote_copy(
            src_ref=base_tx,
            dst_ref=base_rx,
            send_sem=base_sem.at[0],
            recv_sem=base_sem.at[1],
            device_id=above,
            device_id_type=MESH,
        )

    def noise_copy(j, r, slot):
        q, device = mate(r)
        return pltpu.make_async_remote_copy(
            src_ref=noise_v.at[q * own + j],
            dst_ref=noise_all.at[slot, j],
            send_sem=noise_send.at[j, r],
            recv_sem=noise_recv.at[slot, j],
            device_id=device,
            device_id_type=MESH,
        )

    depth = patches // PIECES

    def out_copy(j, r, slot, piece):
        q, device = mate(r)
        cut = pl.ds(piece * depth, depth)
        return pltpu.make_async_remote_copy(
            src_ref=out_tx.at[j, q, cut],
            dst_ref=out_v.at[slot * own + j, cut],
            send_sem=out_send.at[j, r, piece],
            recv_sem=out_recv.at[slot, j, piece],
            device_id=device,
            device_id_type=MESH,
        )

    def chain_copy(n, j, q):
        cut = pl.ds(q * depth, depth)
        return pltpu.make_async_remote_copy(
            src_ref=chain_tx.at[n, j, cut],
            dst_ref=chain_rx.at[n, j, cut],
            send_sem=chain_send.at[n, j, q],
            recv_sem=chain_recv.at[n, j, q],
            device_id=above,
            device_id_type=MESH,
        )

    def late_copy(i, src, dst, device):
        return pltpu.make_async_remote_copy(
            src_ref=src,
            dst_ref=dst,
            send_sem=late_send.at[i],
            recv_sem=late_recv.at[i],
            device_id=device,
            device_id_type=MESH,
        )

    def late_move(i, slot):
        beside, over = {"inner": 1 - h}, {"steps": z * columns + 1 - y}
        if i == 0:
            return late_copy(0, noise_v.at[(other + 1 - h) * own + late], pair_rx, beside)
        if i == 1:
            return late_copy(
                1, noise_v.at[partner * own + late], noise_all.at[slot, late], beside
            )
        return late_copy(i, *((sum_tx, sum_rx) if i == 2 else (raw_tx, raw_rx)), over)

    plain = [j for j in range(own) if j != late]
    for r in range(1, plane):
        gap_copy(r, p).start()
    loads[0].wait()
    for j in plain:
        for r in range(1, plane):
            noise_copy(j, r, p).start()
    if late is not None:
        for i in (0, 1):
            late_move(i, p).start()

    def cut_columns(value):
        return [value[..., i : i + BLOCK] for i in range(0, value.shape[-1], BLOCK)]

    def pack(partial):
        row = lax.broadcasted_iota(jnp.int32, (8, BLOCK), 0)
        top, late = row < 4, lax.rem(row, 4) >= 2
        packed = []
        for i in range(0, partial.shape[0], 4):
            a, b, c, d = (partial[i + k] for k in range(4))
            ab = jnp.where(top, a, b) + pltpu.roll(jnp.where(top, b, a), 4, 0)
            cd = jnp.where(top, c, d) + pltpu.roll(jnp.where(top, d, c), 4, 0)
            four = jnp.where(late, ab + pltpu.roll(ab, 2, 0), cd + pltpu.roll(cd, 6, 0))
            packed.append(four + pltpu.roll(four, 1, 0))
        return packed

    def group_averages(partials):
        size = partials[0].shape[0]
        whole = size % 4 == 0
        rows = []
        for partial in partials:
            rows.extend(pack(partial) if whole else [partial.reshape(size * 8, BLOCK)])
        rows = jnp.concatenate(rows, axis=0)
        high = rows.astype(BF16).astype(F32)
        rest = rows - high
        middle = rest.astype(BF16).astype(F32)
        parts = jnp.concatenate([rest - middle, middle, high], axis=0).astype(BF16)
        summed = jnp.dot(parts, group_ref[...], preferred_element_type=F32)
        summed = jnp.sum(summed.reshape(3, len(partials), -1, BLOCK), axis=0)
        if not whole:
            summed = summed.reshape(len(partials), size, 8, BLOCK)
            return list(jnp.sum(summed, axis=2, keepdims=True))
        places = [i // 4 * 8 + (3, 7, 1, 5)[i % 4] for i in range(size)]
        return [jnp.stack([block[r : r + 1] for r in places], axis=0) for block in summed]

    def row_sums(value):
        size = value.shape[0]
        return jnp.sum(value.reshape(size, patches // 8, 8, BLOCK), axis=1)

    def pivots(block):
        rows = block[:, 0, :]
        lane = lax.broadcasted_iota(jnp.int32, (rows.shape[0], LANES), 1)
        lead = lane - lax.rem(lane, channels // GROUPS)
        halves = [
            jnp.take_along_axis(rows[:, i : i + LANES], lead, axis=1)
            for i in range(0, BLOCK, LANES)
        ]
        return jnp.concatenate(halves, axis=1)[:, None, :]

    def centered(block):
        shifted = block - pivots(block)
        mean, square = group_averages([row_sums(shifted), row_sums(shifted * shifted)])
        return shifted, mean, lax.rsqrt(jnp.maximum(square - mean * mean, 0.0) + 1e-05)

    def project(acts, weight, outer=True):
        sums = [None] * (weight.shape[1] // BLOCK)
        pairs = [(k, n) for k in range(len(acts)) for n in range(len(sums))]
        if not outer:
            pairs = [(k, n) for n in range(len(sums)) for k in range(len(acts))]
        for k, n in pairs:
            tile = weight[pl.ds(k * BLOCK, BLOCK), pl.ds(n * BLOCK, BLOCK)]
            part = jnp.dot(acts[k], tile, preferred_element_type=F32)
            sums[n] = part if sums[n] is None else sums[n] + part
        return sums

    def shape_images(blocks, size):
        return [block.reshape(size, patches, BLOCK) for block in blocks]

    def flatten(value):
        return value.reshape(-1, BLOCK).astype(BF16)

    def activate(blocks):
        result = []
        for block in blocks:
            shifted, mean, spread = centered(block)
            gain = 0.5 * spread
            result.append(flatten(silu_of_half(shifted * gain - mean * gain)))
        return result

    def set_levels():
        for r in range(1, plane):
            slot = mate(r)[0]
            gap_copy(r, slot).wait_recv()

        @pl.when(z > 0)
        def _():
            base_copy().wait_recv()

        gaps = [gap_all[t] for t in range(plane)]
        base = base_rx[...]
        total = base
        for gap in gaps:
            total = total + gap
        base_tx[...] = total

        @pl.when(z < rows - 1)
        def _():
            base_copy().start()

        for i in (8, 9):
            loads[i].wait()
        table = table_ref[...]
        tall = lax.broadcasted_iota(jnp.int32, table.shape, 0)
        places = tall * LANES + lax.broadcasted_iota(jnp.int32, table.shape, 1)
        level = start_level_ref[0] - base
        levels = [level]
        for gap in gaps:
            level = level - gap
            levels.append(level)

        def lookup(level):
            found = jnp.where(places == level[:1, :1], table, 0.0)
            return jnp.sum(jnp.sum(found, axis=0, keepdims=True), axis=1, keepdims=True)

        bars = [lookup(level) for level in levels]
        bar_now, bar_next = jnp.ones(table.shape, F32), jnp.ones(table.shape, F32)
        level_now = levels[0]
        for t in range(plane):
            bar_now = jnp.where(tall == t, bars[t], bar_now)
            bar_next = jnp.where(tall == t, bars[t + 1], bar_next)
            level_now = jnp.where(tall == t, levels[t], level_now)
        rest = 1.0 - bar_now
        lift = (1.0 - bar_next) * jnp.sqrt(bar_now / (bar_next * rest)) / jnp.sqrt(rest)
        coefs = [
            1.0 / jnp.sqrt(bar_now),
            jnp.sqrt(rest) / jnp.sqrt(bar_now),
            jnp.sqrt(bar_next) - lift * jnp.sqrt(bar_now),
            lift - 1.0,
            jnp.sqrt((1.0 - bar_next) / rest * (1.0 - bar_now / bar_next)),
        ]
        for i, coef in enumerate(coefs):
            coef_v[i] = coef
        angles = level_now.astype(F32) * freq_ref[...]
        around = jnp.concatenate([jnp.cos(angles), jnp.sin(angles)], axis=1).astype(BF16)
        loads[4].wait()
        modulation_v[...] = jnp.dot(around, wemb[...], preferred_element_type=F32)

    def modulations(low):
        cut = pl.ds(low, BLOCK)
        return jnp.concatenate(
            [modulation_v[t : t + 1, cut] for t in range(plane)], axis=0
        ).reshape(plane, 1, BLOCK)

    def noise_of(n, j, t):
        if j != late:
            return coef_v[4][t : t + 1, :1] * noise_all[t, j]
        return late_v[t] if n else None

    def drifts(n, j, eps):
        result = []
        for t in range(plane):
            state = start_v[j] if n == 0 else state_v[j, t]
            coef = [coef_v[i][t : t + 1, :1] for i in range(4)]
            clean = jnp.clip(state * coef[0] - eps[t] * coef[1], -1.0, 1.0)
            drift = coef[2] * clean + coef[3] * state
            noise = noise_of(n, j, t)
            result.append(drift if noise is None else drift + noise)
        return result

    def weight(slot):
        return coef_v[4, pl.ds(slot, 1), :1]

    def blend():
        late_move(0, p).wait_recv()
        mine, theirs = noise_v[across * own + late], pair_rx[...]
        sum_tx[...] = weight(p) * mine + weight(partner) * theirs
        raw_tx[...] = jnp.where(h == 0, mine, theirs)
        for i in (2, 3):
            late_move(i, p).start()

    def launch(n, j):
        @pl.when(z == 0)
        def _():
            for q in range(PIECES):
                chain_copy(n, j, q).start()

    def forward(n, j, q):
        @pl.when(z > 0)
        def _():
            cut = pl.ds(q * depth, depth)
            chain_copy(n, j, q).wait_recv()
            chain_tx[n, j, cut] = chain_tx[n, j, cut] + chain_rx[n, j, cut]

            @pl.when(z < rows - 1)
            def _():
                chain_copy(n, j, q).start()

    def denoise(entries, norms, hook, outer):
        images, times = entries[0].shape[:2]
        count = images * plane
        ones = []
        for i, (shifted, mean, spread) in enumerate(norms):
            scale, shift = modulations(i * BLOCK), modulations(channels + i * BLOCK)
            gain = spread * (0.5 + 0.5 * scale[None])
            ones.append(flatten(silu_of_half(shifted * gain + (0.5 * shift[None] - mean * gain))))
        hook(0)
        twos = activate(shape_images(project(ones, w1, outer), count))
        hook(1)
        blocks = []
        for entry, extra in zip(entries, project(twos, w2, outer)):
            total = entry + extra.reshape(images, plane, patches, BLOCK)
            blocks.append(total.reshape(count, patches, BLOCK))
        threes = activate(blocks)
        hook(2)
        eps = jnp.concatenate(project(threes, wout, outer), axis=1)
        hook(3)
        return eps.reshape(images, plane, patches, features)

    def entrance(flat, images, times, outer):
        count = images * times
        blocks = shape_images(project(cut_columns(flat), win, outer), count)
        entries = [block.reshape(images, times, patches, BLOCK) for block in blocks]
        norms = []
        for block in blocks:
            shifted, mean, spread = centered(block)
            stats = (value.reshape(images, times, 1, BLOCK) for value in (mean, spread))
            norms.append((shifted.reshape(images, times, patches, BLOCK), *stats))
        return entries, norms

    def finish_first(j, eps):
        if j == 0:
            loads[3].wait()
        if j != late:
            for r in range(1, plane):
                slot = mate(r)[0]
                noise_copy(j, r, slot).wait_recv()
        parts = drifts(0, j, eps)
        running = parts[0]
        for t in range(1, plane):
            part_v[j, t] = running
            running = running + parts[t]
        if j == late:
            for i in (1, 2):
                late_move(i, partner).wait_recv()
            near = y * inner
            for i in range(inner):
                late_v[near + i] = weight(near + i) * noise_all[near + i, late]
            running = running + (late_v[near] + late_v[near + 1] + sum_rx[...])
        chain_tx[0, j] = running
        launch(0, j)

    def finish_late():
        late_move(3, partner).wait_recv()
        lead = weight(other) * raw_rx[...]
        late_v[other] = lead
        late_v[other + 1] = sum_rx[...] - lead
        running = late_v[0]
        for t in range(1, plane):
            part_v[late, t] = part_v[late, t] + running
            running = running + late_v[t]

    def second(j, hook):
        if j == late:
            finish_late()
        state_v[j, 0] = start_v[j] + chain_rx[0, j]
        for t in range(1, plane):
            state_v[j, t] = start_v[j] + (chain_rx[0, j] + part_v[j, t])
        flat = state_v[j].reshape(plane * patches, features).astype(BF16)
        eps = denoise(*entrance(flat, 1, plane, OUTER_TWO), hook, OUTER_TWO)[0]
        parts = drifts(1, j, eps)
        running = parts[0]
        origin = start_v[j]
        out_tx[j, 0] = origin + running
        for t in range(1, plane):
            running = running + parts[t]
            out_tx[j, t] = origin + running
        chain_tx[1, j] = running
        launch(1, j)
        for q in range(PIECES):
            forward(1, j, q)
            cut = pl.ds(q * depth, depth)
            for t in range(plane):
                out_tx[j, t, cut] = out_tx[j, t, cut] + chain_rx[1, j, cut]
            for r in range(1, plane):
                out_copy(j, r, p, q).start()
        out_v[first + j] = out_tx[j, p]

    for i in (1, 2, 10):
        loads[i].wait()
    flat = start_v[...].reshape(own * patches, features).astype(BF16)
    entries, norms = entrance(flat, own, 1, OUTER_ONE)
    set_levels()
    for i in (5, 6, 7):
        loads[i].wait()

    def idle(stage):
        pass

    if late is not None:
        blend()
    eps = denoise(entries, norms, idle, OUTER_ONE)
    for j in range(1, own):
        eps_v[j - 1] = eps[j]
    finish_first(0, eps[0])

    for q in range(PIECES):
        forward(0, 0, q)
    for j in range(1, own):

        @pl.when(z > 0)
        def _():
            finish_first(j, eps_v[j - 1])

        def relay(stage):
            if stage == LATE_STAGE:

                @pl.when(z == 0)
                def _():
                    finish_first(j, eps_v[j - 1])

            for q in RELAY.get(stage, ()):
                forward(0, j, q)

        second(j - 1, relay)

    second(own - 1, idle)

    for r in range(1, plane):
        slot = mate(r)[0]
        for j in range(own):
            for q in range(PIECES):
                out_copy(j, r, slot, q).wait_recv()

    for r in range(1, plane):
        gap_copy(r, p).wait_send()
        for j in plain:
            noise_copy(j, r, p).wait_send()
        for j in range(own):
            for q in range(PIECES):
                out_copy(j, r, p, q).wait_send()
    if late is not None:
        for i in range(4):
            late_move(i, p).wait_send()

    @pl.when(z < rows - 1)
    def _():
        base_copy().wait_send()
        for n in range(ITERS):
            for j in range(own):
                for q in range(PIECES):
                    chain_copy(n, j, q).wait_send()


def shards(
    steps,
    inner,
    start_state,
    noise_draws,
    step_gaps,
    window_start,
    input_weight,
    embed_weight,
    first_weight,
    second_weight,
    output_weight,
):
    batch, patches, features = start_state.shape
    channels = input_weight.shape[1]
    columns = 2 if steps % 2 == 0 else 1
    plane = columns * inner
    own = batch // plane
    cfg = (steps, inner, columns, own, patches, features, channels)
    image = (patches, features)
    table = jnp.asarray(noise_table())
    freq = jnp.asarray(frequencies(embed_weight.shape[0] // 2))
    matrix = jnp.asarray(group_matrix(channels, patches)).astype(BF16)
    vmem = pl.BlockSpec(memory_space=pltpu.VMEM)
    anywhere = pl.BlockSpec(memory_space=pltpu.HBM)
    dma = pltpu.SemaphoreType.DMA
    out = pl.pallas_call(
        functools.partial(kernel, cfg),
        out_shape=pltpu.VMEM((batch,) + image, F32),
        in_specs=[pl.BlockSpec(memory_space=pltpu.SMEM)] * 2 + [anywhere] * 10,
        out_specs=vmem,
        scratch_shapes=[
            pltpu.VMEM(table.shape, F32),
            pltpu.VMEM(freq.shape, F32),
            pltpu.VMEM(matrix.shape, BF16),
            pltpu.VMEM((own,) + image, F32),
            pltpu.VMEM((batch,) + image, F32),
            pltpu.VMEM((plane, own) + image, F32),
            pltpu.VMEM(input_weight.shape, BF16),
            pltpu.VMEM(embed_weight.shape, BF16),
            pltpu.VMEM(first_weight.shape, BF16),
            pltpu.VMEM(second_weight.shape, BF16),
            pltpu.VMEM(output_weight.shape, BF16),
            pltpu.VMEM((8, LANES), jnp.int32),
            pltpu.VMEM((plane, 8, LANES), jnp.int32),
            pltpu.VMEM((8, LANES), jnp.int32),
            pltpu.VMEM((8, LANES), jnp.int32),
            pltpu.VMEM((8, 2 * channels), F32),
            pltpu.VMEM((5, 8, LANES), F32),
            pltpu.VMEM((own, plane) + image, F32),
            pltpu.VMEM((own, plane) + image, F32),
            pltpu.VMEM((ITERS, own) + image, F32),
            pltpu.VMEM((ITERS, own) + image, F32),
            pltpu.VMEM((own, plane) + image, F32),
            pltpu.VMEM((max(own - 1, 1), plane) + image, F32),
        ]
        + [pltpu.VMEM(image, F32)] * 5
        + [
            pltpu.VMEM((plane,) + image, F32),
            dma((11,)),
            dma((plane,)),
            dma((plane,)),
            dma((2,)),
            dma((own, plane)),
            dma((plane, own)),
            dma((ITERS, own, PIECES)),
            dma((ITERS, own, PIECES)),
            dma((own, plane, PIECES)),
            dma((plane, own, PIECES)),
            dma((4,)),
            dma((4,)),
        ],
        compiler_params=pltpu.CompilerParams(
            collective_id=0, has_side_effects=True, vmem_limit_bytes=56 * 1024 * 1024
        ),
    )(
        step_gaps,
        window_start,
        table,
        freq,
        matrix,
        start_state,
        noise_draws.reshape((batch,) + image),
        input_weight,
        embed_weight,
        first_weight,
        second_weight,
        output_weight,
    )
    return out.reshape((1,) + start_state.shape)


def solution(mesh):
    steps, inner = mesh.shape["steps"], mesh.shape["inner"]
    return jax.shard_map(
        functools.partial(shards, steps, inner),
        mesh=mesh,
        in_specs=(
            P("groups", None, None),
            P(("groups", "steps", "inner"), None, None, None),
            P(("groups", "steps", "inner")),
            P("groups"),
            P(),
            P(),
            P(),
            P(),
            P(),
        ),
        out_specs=P(("groups", "steps", "inner"), None, None, None),
        check_vma=False,
    )
```

```python
import functools
import math

import jax
import jax.numpy as jnp
import numpy as np
from jax import lax
from jax.experimental import pallas as pl
from jax.experimental.pallas import tpu as pltpu
from jax.sharding import PartitionSpec as P

GROUPS = 32
PIECES = 4
OUTER_ONE = False
OUTER_TWO = False
ITERS = 2
TRAIN_STEPS = 1000
LANES = 128
BLOCK = 256
MESH = pl.DeviceIdType.MESH
F32 = jnp.float32
BF16 = jnp.bfloat16


def noise_table():
    levels = np.arange(TRAIN_STEPS, dtype=np.float32)
    beta = (0.0001 + (0.02 - 0.0001) * levels / (TRAIN_STEPS - 1)).astype(np.float32)
    bars = np.exp(np.cumsum(np.log1p(-beta.astype(np.float64)))).astype(np.float32)
    padded = np.zeros((-(-TRAIN_STEPS // (8 * LANES)) * 8 * LANES,), np.float32)
    padded[:TRAIN_STEPS] = bars
    return padded.reshape(-1, LANES)


def frequencies(count):
    powers = -math.log(10000.0) * np.arange(count, dtype=np.float32) / count
    return np.exp(powers.astype(np.float32)).astype(np.float32)[None, :]


def group_matrix(channels, rows):
    width = channels // GROUPS
    place = np.arange(BLOCK) // width
    same = (place[:, None] == place[None, :]).astype(np.float32)
    return same / (width * rows)


def silu_of_half(half):
    return half + half * jnp.tanh(half)


def kernel(
    cfg,
    gap_hbm,
    start_level_hbm,
    table_hbm,
    freq_hbm,
    group_hbm,
    start_hbm,
    noise_hbm,
    win_hbm,
    wemb_hbm,
    w1_hbm,
    w2_hbm,
    wout_hbm,
    out_v,
    gap_ref,
    start_level_ref,
    table_ref,
    freq_ref,
    group_ref,
    start_v,
    noise_v,
    noise_all,
    win,
    wemb,
    w1,
    w2,
    wout,
    gap_send,
    gap_all,
    base_rx,
    base_tx,
    modulation_v,
    coef_v,
    part_v,
    state_v,
    chain_rx,
    chain_tx,
    out_tx,
    eps_v,
    pair_rx,
    sum_tx,
    sum_rx,
    raw_tx,
    raw_rx,
    late_v,
    load_sem,
    gap_send_sem,
    gap_recv_sem,
    base_sem,
    noise_send,
    noise_recv,
    chain_send,
    chain_recv,
    out_send,
    out_recv,
    late_send,
    late_recv,
):
    steps, inner, columns, own, patches, features, channels = cfg
    rows = steps // columns
    plane = columns * inner
    s = lax.axis_index("steps")
    h = lax.axis_index("inner")
    z = s // columns
    y = lax.rem(s, columns)
    p = y * inner + h
    first = p * own
    late = own - 1 if own > 1 and columns == 2 and inner == 2 else None
    partner, across, other = p + 1 - 2 * h, (1 - y) * inner + h, (1 - y) * inner

    def load(i, src, dst):
        return pltpu.make_async_copy(src, dst, load_sem.at[i])

    loads = [
        load(0, noise_hbm, noise_v),
        load(1, start_hbm.at[pl.ds(first, own)], start_v),
        load(2, win_hbm, win),
        load(3, noise_hbm.at[pl.ds(first, own)], noise_all.at[p]),
        load(4, wemb_hbm, wemb),
        load(5, w1_hbm, w1),
        load(6, w2_hbm, w2),
        load(7, wout_hbm, wout),
        load(8, gap_hbm, gap_ref),
        load(9, start_level_hbm, start_level_ref),
        load(10, table_hbm, table_ref),
        load(11, freq_hbm, freq_ref),
        load(12, group_hbm, group_ref),
    ]
    def mate(r):
        q = lax.rem(p + r, plane)
        return q, {"steps": z * columns + q // inner, "inner": lax.rem(q, inner)}

    below, above = {"steps": s - columns}, {"steps": s + columns}

    barrier = pltpu.get_barrier_semaphore()
    for r in range(1, plane):
        pl.semaphore_signal(barrier, inc=1, device_id=mate(r)[1], device_id_type=MESH)

    @pl.when(z > 0)
    def _():
        pl.semaphore_signal(barrier, inc=1, device_id=below, device_id_type=MESH)

    for i in (8, 0, 9, 10, 11, 1, 2, 12, 3, 4, 5, 6, 7):
        loads[i].start()

    loads[8].wait()
    gap_send[...] = jnp.zeros_like(gap_send) + gap_ref[0]
    gap_all[p] = jnp.zeros_like(gap_send) + gap_ref[0]

    @pl.when(z == 0)
    def _():
        base_rx[...] = jnp.zeros_like(base_rx)
        chain_rx[...] = jnp.zeros_like(chain_rx)

    neighbours = (2 * rows - 2 - z) // rows
    pl.semaphore_wait(barrier, plane - 1 + neighbours)

    def gap_copy(r, slot):
        return pltpu.make_async_remote_copy(
            src_ref=gap_send,
            dst_ref=gap_all.at[slot],
            send_sem=gap_send_sem.at[r],
            recv_sem=gap_recv_sem.at[slot],
            device_id=mate(r)[1],
            device_id_type=MESH,
        )

    def base_copy():
        return pltpu.make_async_remote_copy(
            src_ref=base_tx,
            dst_ref=base_rx,
            send_sem=base_sem.at[0],
            recv_sem=base_sem.at[1],
            device_id=above,
            device_id_type=MESH,
        )

    def noise_copy(j, r, slot):
        q, device = mate(r)
        return pltpu.make_async_remote_copy(
            src_ref=noise_v.at[q * own + j],
            dst_ref=noise_all.at[slot, j],
            send_sem=noise_send.at[j, r],
            recv_sem=noise_recv.at[slot, j],
            device_id=device,
            device_id_type=MESH,
        )

    depth = patches // PIECES

    def out_copy(j, r, slot, piece):
        q, device = mate(r)
        cut = pl.ds(piece * depth, depth)
        return pltpu.make_async_remote_copy(
            src_ref=out_tx.at[j, q, cut],
            dst_ref=out_v.at[slot * own + j, cut],
            send_sem=out_send.at[j, r, piece],
            recv_sem=out_recv.at[slot, j, piece],
            device_id=device,
            device_id_type=MESH,
        )

    def chain_copy(n, j, q):
        cut = pl.ds(q * depth, depth)
        return pltpu.make_async_remote_copy(
            src_ref=chain_tx.at[n, j, cut],
            dst_ref=chain_rx.at[n, j, cut],
            send_sem=chain_send.at[n, j, q],
            recv_sem=chain_recv.at[n, j, q],
            device_id=above,
            device_id_type=MESH,
        )

    def late_copy(i, src, dst, device):
        return pltpu.make_async_remote_copy(
            src_ref=src,
            dst_ref=dst,
            send_sem=late_send.at[i],
            recv_sem=late_recv.at[i],
            device_id=device,
            device_id_type=MESH,
        )

    def late_move(i, slot):
        beside, over = {"inner": 1 - h}, {"steps": z * columns + 1 - y}
        if i == 0:
            return late_copy(0, noise_v.at[(other + 1 - h) * own + late], pair_rx, beside)
        if i == 1:
            return late_copy(
                1, noise_v.at[partner * own + late], noise_all.at[slot, late], beside
            )
        return late_copy(i, *((sum_tx, sum_rx) if i == 2 else (raw_tx, raw_rx)), over)

    plain = [j for j in range(own) if j != late]
    order = sorted(range(1, plane), key=lambda r: r % inner)
    for r in range(1, plane):
        gap_copy(r, p).start()
    loads[0].wait()
    for j in plain:
        for r in order:
            noise_copy(j, r, p).start()
    if late is not None:
        for i in (0, 1):
            late_move(i, p).start()

    def cut_columns(value):
        return [value[..., i : i + BLOCK] for i in range(0, value.shape[-1], BLOCK)]

    def pack(partial):
        row = lax.broadcasted_iota(jnp.int32, (8, BLOCK), 0)
        top, late = row < 4, lax.rem(row, 4) >= 2
        packed = []
        for i in range(0, partial.shape[0], 4):
            a, b, c, d = (partial[i + k] for k in range(4))
            ab = jnp.where(top, a, b) + pltpu.roll(jnp.where(top, b, a), 4, 0)
            cd = jnp.where(top, c, d) + pltpu.roll(jnp.where(top, d, c), 4, 0)
            four = jnp.where(late, ab + pltpu.roll(ab, 2, 0), cd + pltpu.roll(cd, 6, 0))
            packed.append(four + pltpu.roll(four, 1, 0))
        return packed

    def group_averages(partials):
        size = partials[0].shape[0]
        whole = size % 4 == 0
        rows = []
        for partial in partials:
            rows.extend(pack(partial) if whole else [partial.reshape(size * 8, BLOCK)])
        rows = jnp.concatenate(rows, axis=0)
        high = rows.astype(BF16).astype(F32)
        rest = rows - high
        middle = rest.astype(BF16).astype(F32)
        parts = jnp.concatenate([rest - middle, middle, high], axis=0).astype(BF16)
        summed = jnp.dot(parts, group_ref[...], preferred_element_type=F32)
        summed = jnp.sum(summed.reshape(3, len(partials), -1, BLOCK), axis=0)
        if not whole:
            summed = summed.reshape(len(partials), size, 8, BLOCK)
            return list(jnp.sum(summed, axis=2, keepdims=True))
        places = [i // 4 * 8 + (3, 7, 1, 5)[i % 4] for i in range(size)]
        return [jnp.stack([block[r : r + 1] for r in places], axis=0) for block in summed]

    def row_sums(value):
        size = value.shape[0]
        return jnp.sum(value.reshape(size, patches // 8, 8, BLOCK), axis=1)

    def pivots(block):
        rows = block[:, 0, :]
        lane = lax.broadcasted_iota(jnp.int32, (rows.shape[0], LANES), 1)
        lead = lane - lax.rem(lane, channels // GROUPS)
        halves = [
            jnp.take_along_axis(rows[:, i : i + LANES], lead, axis=1)
            for i in range(0, BLOCK, LANES)
        ]
        return jnp.concatenate(halves, axis=1)[:, None, :]

    def centered(block):
        shifted = block - pivots(block)
        mean, square = group_averages([row_sums(shifted), row_sums(shifted * shifted)])
        return shifted, mean, lax.rsqrt(jnp.maximum(square - mean * mean, 0.0) + 1e-05)

    def project(acts, weight, outer=True):
        sums = [None] * (weight.shape[1] // BLOCK)
        pairs = [(k, n) for k in range(len(acts)) for n in range(len(sums))]
        if not outer:
            pairs = [(k, n) for n in range(len(sums)) for k in range(len(acts))]
        for k, n in pairs:
            tile = weight[pl.ds(k * BLOCK, BLOCK), pl.ds(n * BLOCK, BLOCK)]
            part = jnp.dot(acts[k], tile, preferred_element_type=F32)
            sums[n] = part if sums[n] is None else sums[n] + part
        return sums

    def shape_images(blocks, size):
        return [block.reshape(size, patches, BLOCK) for block in blocks]

    def flatten(value):
        return value.reshape(-1, BLOCK).astype(BF16)

    def activate(blocks):
        result = []
        for block in blocks:
            shifted, mean, spread = centered(block)
            gain = 0.5 * spread
            result.append(flatten(silu_of_half(shifted * gain - mean * gain)))
        return result

    def set_levels():
        for r in range(1, plane):
            slot = mate(r)[0]
            gap_copy(r, slot).wait_recv()

        @pl.when(z > 0)
        def _():
            base_copy().wait_recv()

        gaps = [gap_all[t] for t in range(plane)]
        base = base_rx[...]
        total = base
        for gap in gaps:
            total = total + gap
        base_tx[...] = total

        @pl.when(z < rows - 1)
        def _():
            base_copy().start()

        for i in (9, 10, 11):
            loads[i].wait()
        table = table_ref[...]
        tall = lax.broadcasted_iota(jnp.int32, table.shape, 0)
        places = tall * LANES + lax.broadcasted_iota(jnp.int32, table.shape, 1)
        level = start_level_ref[0] - base
        levels = [level]
        for gap in gaps:
            level = level - gap
            levels.append(level)

        def lookup(level):
            found = jnp.where(places == level[:1, :1], table, 0.0)
            return jnp.sum(jnp.sum(found, axis=0, keepdims=True), axis=1, keepdims=True)

        bars = [lookup(level) for level in levels]
        bar_now, bar_next = jnp.ones(table.shape, F32), jnp.ones(table.shape, F32)
        level_now = levels[0]
        for t in range(plane):
            bar_now = jnp.where(tall == t, bars[t], bar_now)
            bar_next = jnp.where(tall == t, bars[t + 1], bar_next)
            level_now = jnp.where(tall == t, levels[t], level_now)
        rest = 1.0 - bar_now
        lift = (1.0 - bar_next) * jnp.sqrt(bar_now / (bar_next * rest)) / jnp.sqrt(rest)
        coefs = [
            1.0 / jnp.sqrt(bar_now),
            jnp.sqrt(rest) / jnp.sqrt(bar_now),
            jnp.sqrt(bar_next) - lift * jnp.sqrt(bar_now),
            lift - 1.0,
            jnp.sqrt((1.0 - bar_next) / rest * (1.0 - bar_now / bar_next)),
        ]
        for i, coef in enumerate(coefs):
            coef_v[i] = coef
        angles = level_now.astype(F32) * freq_ref[...]
        around = jnp.concatenate([jnp.cos(angles), jnp.sin(angles)], axis=1).astype(BF16)
        loads[4].wait()
        modulation_v[...] = jnp.dot(around, wemb[...], preferred_element_type=F32)

    def modulations(low):
        cut = pl.ds(low, BLOCK)
        return jnp.concatenate(
            [modulation_v[t : t + 1, cut] for t in range(plane)], axis=0
        ).reshape(plane, 1, BLOCK)

    def noise_of(n, j, t):
        if j != late:
            return coef_v[4][t : t + 1, :1] * noise_all[t, j]
        return late_v[t] if n else None

    def drifts(n, j, eps):
        result = []
        for t in range(plane):
            state = start_v[j] if n == 0 else state_v[j, t]
            coef = [coef_v[i][t : t + 1, :1] for i in range(4)]
            clean = jnp.clip(state * coef[0] - eps[t] * coef[1], -1.0, 1.0)
            drift = coef[2] * clean + coef[3] * state
            noise = noise_of(n, j, t)
            result.append(drift if noise is None else drift + noise)
        return result

    def weight(slot):
        return coef_v[4, pl.ds(slot, 1), :1]

    def blend():
        late_move(0, p).wait_recv()
        mine, theirs = noise_v[across * own + late], pair_rx[...]
        sum_tx[...] = weight(p) * mine + weight(partner) * theirs
        raw_tx[...] = jnp.where(h == 0, mine, theirs)
        for i in (2, 3):
            late_move(i, p).start()

    def launch(n, j):
        @pl.when(z == 0)
        def _():
            for q in range(PIECES):
                chain_copy(n, j, q).start()

    def forward(n, j, q):
        @pl.when(z > 0)
        def _():
            cut = pl.ds(q * depth, depth)
            chain_copy(n, j, q).wait_recv()

            @pl.when(z < rows - 1)
            def _():
                chain_tx[n, j, cut] = chain_tx[n, j, cut] + chain_rx[n, j, cut]
                chain_copy(n, j, q).start()

    def denoise(entries, norms, hook, outer):
        images, times = entries[0].shape[:2]
        count = images * plane
        ones = []
        for i, (shifted, mean, spread) in enumerate(norms):
            scale, shift = modulations(i * BLOCK), modulations(channels + i * BLOCK)
            gain = spread * (0.5 + 0.5 * scale[None])
            ones.append(flatten(silu_of_half(shifted * gain + (0.5 * shift[None] - mean * gain))))
        hook(0)
        twos = activate(shape_images(project(ones, w1, outer), count))
        hook(1)
        blocks = []
        for entry, extra in zip(entries, project(twos, w2, outer)):
            total = entry + extra.reshape(images, plane, patches, BLOCK)
            blocks.append(total.reshape(count, patches, BLOCK))
        threes = activate(blocks)
        hook(2)
        eps = jnp.concatenate(project(threes, wout, outer), axis=1)
        hook(3)
        return eps.reshape(images, plane, patches, features)

    def entrance(flat, images, times, outer):
        count = images * times
        blocks = shape_images(project(cut_columns(flat), win, outer), count)
        entries = [block.reshape(images, times, patches, BLOCK) for block in blocks]
        norms = []
        for block in blocks:
            shifted, mean, spread = centered(block)
            stats = (value.reshape(images, times, 1, BLOCK) for value in (mean, spread))
            norms.append((shifted.reshape(images, times, patches, BLOCK), *stats))
        return entries, norms

    def finish_first(j, eps):
        if j == 0:
            loads[3].wait()
        if j != late:
            for r in range(1, plane):
                slot = mate(r)[0]
                noise_copy(j, r, slot).wait_recv()
        parts = drifts(0, j, eps)
        running = parts[0]
        for t in range(1, plane):
            part_v[j, t] = running
            running = running + parts[t]
        if j == late:
            for i in (1, 2):
                late_move(i, partner).wait_recv()
            near = y * inner
            for i in range(inner):
                late_v[near + i] = weight(near + i) * noise_all[near + i, late]
            running = running + (late_v[near] + late_v[near + 1] + sum_rx[...])
        chain_tx[0, j] = running
        launch(0, j)

    def finish_late():
        late_move(3, partner).wait_recv()
        lead = weight(other) * raw_rx[...]
        late_v[other] = lead
        late_v[other + 1] = sum_rx[...] - lead
        running = late_v[0]
        for t in range(1, plane):
            part_v[late, t] = part_v[late, t] + running
            running = running + late_v[t]

    def second(j, hook):
        if j == late:
            finish_late()
        state_v[j, 0] = start_v[j] + chain_rx[0, j]
        for t in range(1, plane):
            state_v[j, t] = start_v[j] + (chain_rx[0, j] + part_v[j, t])
        flat = state_v[j].reshape(plane * patches, features).astype(BF16)
        eps = denoise(*entrance(flat, 1, plane, OUTER_TWO), hook, OUTER_TWO)[0]
        parts = drifts(1, j, eps)
        running = parts[0]
        origin = start_v[j]
        out_tx[j, 0] = origin + running
        for t in range(1, plane):
            running = running + parts[t]
            out_tx[j, t] = origin + running
        chain_tx[1, j] = running
        launch(1, j)
        for q in range(PIECES):
            forward(1, j, q)
            cut = pl.ds(q * depth, depth)
            for t in range(plane):
                out_tx[j, t, cut] = out_tx[j, t, cut] + chain_rx[1, j, cut]
            for r in order:
                out_copy(j, r, p, q).start()
        out_v[first + j] = out_tx[j, p]

    for i in (1, 2, 12):
        loads[i].wait()
    flat = start_v[...].reshape(own * patches, features).astype(BF16)
    entries, norms = entrance(flat, own, 1, OUTER_ONE)
    for i in (5, 6, 7):
        loads[i].wait()
    set_levels()

    def idle(stage):
        pass

    if late is not None:
        blend()
    eps = denoise(entries, norms, idle, OUTER_ONE)
    for j in range(1, own):
        eps_v[j - 1] = eps[j]
    finish_first(0, eps[0])

    for q in range(PIECES):
        forward(0, 0, q)
    for j in range(1, own):

        @pl.when(z > 0)
        def _():
            finish_first(j, eps_v[j - 1])

        def relay(stage):
            if stage == 2:

                @pl.when(z == 0)
                def _():
                    finish_first(j, eps_v[j - 1])

            if stage < PIECES:
                forward(0, j, stage)

        second(j - 1, relay)
        for q in range(4, PIECES):
            forward(0, j, q)

    second(own - 1, idle)

    for r in range(1, plane):
        slot = mate(r)[0]
        for j in range(own):
            for q in range(PIECES):
                out_copy(j, r, slot, q).wait_recv()

    for r in range(1, plane):
        gap_copy(r, p).wait_send()
        for j in plain:
            noise_copy(j, r, p).wait_send()
        for j in range(own):
            for q in range(PIECES):
                out_copy(j, r, p, q).wait_send()
    if late is not None:
        for i in range(4):
            late_move(i, p).wait_send()

    @pl.when(z < rows - 1)
    def _():
        base_copy().wait_send()
        for n in range(ITERS):
            for j in range(own):
                for q in range(PIECES):
                    chain_copy(n, j, q).wait_send()


def shards(
    steps,
    inner,
    start_state,
    noise_draws,
    step_gaps,
    window_start,
    input_weight,
    embed_weight,
    first_weight,
    second_weight,
    output_weight,
):
    batch, patches, features = start_state.shape
    channels = input_weight.shape[1]
    columns = 2 if steps % 2 == 0 else 1
    plane = columns * inner
    own = batch // plane
    cfg = (steps, inner, columns, own, patches, features, channels)
    image = (patches, features)
    table = jnp.asarray(noise_table())
    freq = jnp.asarray(frequencies(embed_weight.shape[0] // 2))
    matrix = jnp.asarray(group_matrix(channels, patches)).astype(BF16)
    vmem = pl.BlockSpec(memory_space=pltpu.VMEM)
    anywhere = pl.BlockSpec(memory_space=pltpu.HBM)
    dma = pltpu.SemaphoreType.DMA
    out = pl.pallas_call(
        functools.partial(kernel, cfg),
        out_shape=pltpu.VMEM((batch,) + image, F32),
        in_specs=[anywhere] * 12,
        out_specs=vmem,
        scratch_shapes=[
            pltpu.SMEM((1,), jnp.int32),
            pltpu.SMEM((1,), jnp.int32),
            pltpu.VMEM(table.shape, F32),
            pltpu.VMEM(freq.shape, F32),
            pltpu.VMEM(matrix.shape, BF16),
            pltpu.VMEM((own,) + image, F32),
            pltpu.VMEM((batch,) + image, F32),
            pltpu.VMEM((plane, own) + image, F32),
            pltpu.VMEM(input_weight.shape, BF16),
            pltpu.VMEM(embed_weight.shape, BF16),
            pltpu.VMEM(first_weight.shape, BF16),
            pltpu.VMEM(second_weight.shape, BF16),
            pltpu.VMEM(output_weight.shape, BF16),
            pltpu.VMEM((8, LANES), jnp.int32),
            pltpu.VMEM((plane, 8, LANES), jnp.int32),
            pltpu.VMEM((8, LANES), jnp.int32),
            pltpu.VMEM((8, LANES), jnp.int32),
            pltpu.VMEM((8, 2 * channels), F32),
            pltpu.VMEM((5, 8, LANES), F32),
            pltpu.VMEM((own, plane) + image, F32),
            pltpu.VMEM((own, plane) + image, F32),
            pltpu.VMEM((ITERS, own) + image, F32),
            pltpu.VMEM((ITERS, own) + image, F32),
            pltpu.VMEM((own, plane) + image, F32),
            pltpu.VMEM((max(own - 1, 1), plane) + image, F32),
        ]
        + [pltpu.VMEM(image, F32)] * 5
        + [
            pltpu.VMEM((plane,) + image, F32),
            dma((13,)),
            dma((plane,)),
            dma((plane,)),
            dma((2,)),
            dma((own, plane)),
            dma((plane, own)),
            dma((ITERS, own, PIECES)),
            dma((ITERS, own, PIECES)),
            dma((own, plane, PIECES)),
            dma((plane, own, PIECES)),
            dma((4,)),
            dma((4,)),
        ],
        compiler_params=pltpu.CompilerParams(
            collective_id=0, has_side_effects=True, vmem_limit_bytes=56 * 1024 * 1024
        ),
    )(
        step_gaps,
        window_start,
        table,
        freq,
        matrix,
        start_state,
        noise_draws.reshape((batch,) + image),
        input_weight,
        embed_weight,
        first_weight,
        second_weight,
        output_weight,
    )
    return out.reshape((1,) + start_state.shape)


def solution(mesh):
    steps, inner = mesh.shape["steps"], mesh.shape["inner"]
    return jax.shard_map(
        functools.partial(shards, steps, inner),
        mesh=mesh,
        in_specs=(
            P("groups", None, None),
            P(("groups", "steps", "inner"), None, None, None),
            P(("groups", "steps", "inner")),
            P("groups"),
            P(),
            P(),
            P(),
            P(),
            P(),
        ),
        out_specs=P(("groups", "steps", "inner"), None, None, None),
        check_vma=False,
    )
```
